32 devices in a mesh: dp: 4 (over z), expert: 4 (over y, x), tensor: 2 (over core).
Axes of the slice: x: 2, y: 2, z: 4, core: 2. Of those that a mesh axis runs over, the one named last changes fastest.
Arguments:
- tokens: bfloat16 [192, 7168], P(('dp', 'expert')), may hold values from -6 to 6
- expert_ids: int32 [192, 8], P(('dp', 'expert')), may hold values from 0 to 15, all different within a row; in each aligned block of 12 rows (0 to 11, 12 to 23, ...) at most 8 rows name the same one
- route_weights: float32 [192, 8], P(('dp', 'expert')), may hold values from 0.1 to 1
- gate_weights: bfloat16 [16, 7168, 2048], P('expert', 'dp', 'tensor'), may hold values from -0.0625 to 0.0625
- up_weights: bfloat16 [16, 7168, 2048], P('expert', 'dp', 'tensor'), may hold values from -0.0625 to 0.0625
- down_weights: bfloat16 [16, 2048, 7168], P('expert', 'tensor', 'dp'), may hold values from -0.125 to 0.125
- shared_gate: bfloat16 [7168, 2048], P('dp', 'tensor'), may hold values from -0.0625 to 0.0625
- shared_up: bfloat16 [7168, 2048], P('dp', 'tensor'), may hold values from -0.0625 to 0.0625
- shared_down: bfloat16 [2048, 7168], P('tensor', 'dp'), may hold values from -0.125 to 0.125
Outputs:
- mixed: bfloat16 [192, 7168], P(('dp', 'expert'))
The draws below stay inside these ranges and needn't reach their ends.
Inputs may be any that keep to these rules, and one draw needn't show every extreme that they name: `expert_ids`: each token names 8 different experts. In the rows of one device no expert is named by more than 8 tokens, and in some device's rows some expert is named by exactly 8.
All inputs are finite; a program needn't handle non-finite values.
Results may differ from the reference program's by a relative error of at most 0.005.
Values may be sent and summed in bfloat16 or wider, within the bound.
A program may use at most 128 MiB of HBM per device.

```python
import math
import jax
import jax.numpy as jnp
import numpy as np
from jax import lax

D = 7168
FF = 2048
TOP = 8
EXPERTS = 16
TOK_DEV = 12
CAP = 8
TOKENS = 192


def block_levels(own_key, shape, shards, smallest, high):
    gain, own = 1.0, jax.random.fold_in(own_key, 6)
    for axis_at, shards_of in shards:
        heights = jnp.exp(jax.random.uniform(jax.random.fold_in(own, axis_at), (shards_of,), jnp.float32, smallest / len(shards), high / len(shards)))
        gain = gain * jnp.repeat(heights, shape[axis_at] // shards_of).reshape([-1 if axis == axis_at else 1 for axis in range(len(shape))])
    return gain


def assign_block(stream_key, own, number, rows, amount, top, limit, skew):
    sequence = jax.random.permutation(stream_key, amount)
    packed, common = shares(amount, rows * top, limit, skew, True), shares(amount, rows * top, limit, skew, False)
    places = jnp.arange(amount)

    def named(lengths, offset_by):
        used = int((lengths > 0).sum())
        fixed = max(1, used // 4)
        passed = fixed + (places - fixed + offset_by * (used - fixed)) % max(1, amount - fixed)
        return jnp.zeros((amount,), jnp.int32).at[sequence[jnp.where(places < fixed, places, passed)]].set(jnp.asarray(lengths, jnp.int32))

    lengths = jnp.where(number % 4 == 0, named(packed, number // 4), named(common, number - number // 4 - 1))
    mixed = jax.random.permutation(jax.random.fold_in(own, 3), amount)
    donor, sink = mixed[0:amount // 2 * 2:2], mixed[1:amount // 2 * 2:2]
    margin = jnp.minimum(lengths[donor] - 1, limit - lengths[sink]) // 2
    margin = jnp.where((donor == sequence[0]) | (sink == sequence[0]) | (lengths[sink] == 0), 0, jnp.maximum(margin, 0))
    passed = jax.random.randint(jax.random.fold_in(own, 4), (amount // 2,), 0, 1 << 20) % (margin + 1)
    lengths = lengths.at[donor].add(-passed).at[sink].add(passed)
    labels = jnp.searchsorted(jnp.cumsum(lengths), jnp.arange(rows * top), side="right").astype(jnp.int32)
    table = labels.reshape(top, rows).T
    table = table[jax.random.permutation(jax.random.fold_in(own, 1), rows)]
    offset_by = jax.random.randint(jax.random.fold_in(own, 2), (rows, 1), 0, top)
    return jnp.take_along_axis(table, (jnp.arange(top)[None, :] + offset_by) % top, axis=1)


def shares(number_of, total, limit, lean, full):
    loads = [(1 << 20) // math.isqrt(grade ** lean) + 1 for grade in range(1, number_of + 1)]
    largest = limit if full else min(limit, max(-(-total // number_of), total * loads[0] // sum(loads)))
    least = 1 if total - largest >= number_of - 1 else 0
    counts, spare = [largest] + [least] * (number_of - 1), total - largest - least * (number_of - 1)
    while spare > 0:
        movable = [i for i in range(1, number_of) if counts[i] < largest] or [i for i in range(1, number_of) if counts[i] < limit]
        mass, remaining = sum([loads[i] for i in movable]), spare
        for i in movable:
            addition = min(limit - counts[i], max(1, remaining * loads[i] // mass), spare)
            counts[i] = counts[i] + addition
            spare = spare - addition
    return np.array(counts)


def noise(key, shape, width, limit, cuts=(), kind=jnp.bfloat16):
    gain = block_levels(key, shape, cuts, -0.22, 0.18) if cuts else 1.0
    array = jax.random.normal(key, shape, jnp.float32) * width * gain
    return jnp.minimum(jnp.maximum(array, -limit), limit).astype(kind)


def setup_inputs(seed: int = 0) -> dict:
    key_of = jax.random.split(jax.random.key(seed), 10)
    tokens = noise(key_of[0], (TOKENS, D), 1.0, 6.0, ((0, 16),))
    expert_ids_keys = jax.random.split(jax.random.fold_in(key_of[1], 1), TOKENS // TOK_DEV)
    expert_ids_turns = jax.random.permutation(jax.random.fold_in(key_of[1], 3), TOKENS // TOK_DEV)
    expert_ids = jax.vmap(lambda own, number: assign_block(jax.random.fold_in(key_of[1], 2), own, number, TOK_DEV, EXPERTS, TOP, CAP, 2))(expert_ids_keys, expert_ids_turns).reshape((TOKENS, TOP))
    route_weights = jnp.clip(jnp.exp(math.log(1.0) - 2.3025851 * jax.random.uniform(key_of[2], (TOKENS, TOP), jnp.float32) ** block_levels(key_of[2], (TOKENS, TOP), ((0, 16),), -0.2, 0.2)), 0.1, 1.0)
    gate_weights = noise(key_of[3], (EXPERTS, D, FF), D ** -0.5, 0.0625, ((0, 4), (1, 4), (2, 2)))
    up_weights = noise(key_of[4], (EXPERTS, D, FF), D ** -0.5, 0.0625, ((0, 4), (1, 4), (2, 2)))
    down_weights = noise(key_of[5], (EXPERTS, FF, D), FF ** -0.5, 0.125, ((0, 4), (1, 2), (2, 4)))
    shared_gate = noise(key_of[6], (D, FF), D ** -0.5, 0.0625, ((0, 4), (1, 2)))
    shared_up = noise(key_of[7], (D, FF), D ** -0.5, 0.0625, ((0, 4), (1, 2)))
    shared_down = noise(key_of[8], (FF, D), FF ** -0.5, 0.125, ((0, 2), (1, 4)))
    return dict(tokens=tokens, expert_ids=expert_ids, route_weights=route_weights, gate_weights=gate_weights, up_weights=up_weights, down_weights=down_weights, shared_gate=shared_gate, shared_up=shared_up, shared_down=shared_down)


def reference(tokens, expert_ids, route_weights, gate_weights, up_weights, down_weights, shared_gate, shared_up, shared_down):
    shared_gate_out = jnp.dot(tokens, shared_gate, preferred_element_type=jnp.float32)
    shared_up_out = jnp.dot(tokens, shared_up, preferred_element_type=jnp.float32)
    shared_hidden = (jax.nn.silu(shared_gate_out) * shared_up_out).astype(jnp.bfloat16)
    shared_out = jnp.dot(shared_hidden, shared_down, preferred_element_type=jnp.float32)

    def accumulate(running, layer_pack):
        gate_matrix, up_matrix, down_matrix, expert_index = layer_pack
        gate_out = jnp.dot(tokens, gate_matrix, preferred_element_type=jnp.float32)
        up_out = jnp.dot(tokens, up_matrix, preferred_element_type=jnp.float32)
        hidden = (jax.nn.silu(gate_out) * up_out).astype(jnp.bfloat16)
        expert_out = jnp.dot(hidden, down_matrix, preferred_element_type=jnp.float32)
        coefficient = jnp.sum(jnp.where(expert_ids == expert_index, route_weights, jnp.zeros_like(route_weights)), axis=1)
        return running + coefficient[:, None] * expert_out.astype(running.dtype), None

    indices = jnp.arange(EXPERTS, dtype=jnp.int32)
    running, unused = lax.scan(accumulate, shared_out, (gate_weights, up_weights, down_weights, indices))
    return running.astype(jnp.bfloat16)
```

```python
import functools

import jax
import jax.numpy as jnp
from jax import lax
from jax.experimental import pallas as pl
from jax.experimental.pallas import tpu as pltpu
from jax.sharding import PartitionSpec as P

CAP = 8
PITCH = 16
TILE = 256
COLS = 256
ROWS = 64
AHEAD = 3
SKEW = 2
SPREAD_SKEW = 2
MESH = pl.DeviceIdType.MESH
VMEM = pl.BlockSpec(memory_space=pltpu.VMEM)
HBM = pl.BlockSpec(memory_space=pl.ANY)
DMA = pltpu.SemaphoreType.DMA
F32 = jnp.float32
BF16 = jnp.bfloat16


def greet(peers):
    barrier = pltpu.get_barrier_semaphore()
    for peer in peers:
        pl.semaphore_signal(barrier, inc=1, device_id=peer, device_id_type=MESH)
    pl.semaphore_wait(barrier, len(peers))


def remote(src, dst, send, recv, peer):
    return pltpu.make_async_remote_copy(
        src_ref=src, dst_ref=dst, send_sem=send, recv_sem=recv, device_id=peer, device_id_type=MESH
    )


def params(number, limit=60 * 1024 * 1024):
    return pltpu.CompilerParams(
        collective_id=number, has_side_effects=True, vmem_limit_bytes=limit
    )


def packed(v, wire):
    return v if wire == F32 else (v * jnp.abs(v)).astype(wire)


def unpacked(v):
    if v.dtype == F32:
        return v
    v = v.astype(F32)
    size = jnp.abs(v)
    root = size * lax.rsqrt(jnp.maximum(size, 1e-30))
    return jnp.where(v < 0.0, -root, root)


def dot(a, b):
    return jnp.dot(a, b, preferred_element_type=F32)


def dispatch_kernel(n, g, tok, ids, weights, x, w, coef, own, s1, r1, s2, r2, s3, r3):
    d, e, t = lax.axis_index("dp"), lax.axis_index("expert"), lax.axis_index("tensor")
    width, experts = x.shape[3], w.shape[3]
    split = (width // 2) % 128 == 0
    half = width // 2 if split else width
    lanes = pl.ds(pl.multiple_of(t * half, 128), half) if split else pl.ds(0, width)

    def columns(block, part):
        start = block * width + (t * half if part and split else 0)
        return tok.at[:, pl.ds(pl.multiple_of(start, 128), half if part else width)]

    mine = pltpu.make_async_copy(columns(d, False), x.at[d, e], own.at[0])
    mine.start()
    name = lax.broadcasted_iota(jnp.int32, coef.shape, 1)
    total = jnp.zeros(coef.shape, F32)
    for k in range(ids.shape[1]):
        total = total + jnp.where(ids[:, k:k + 1] == name, weights[:, k:k + 1], 0.0)
    coef[...] = total
    greet(
        [{"dp": lax.rem(d + k, n)} for k in range(1, n)]
        + [{"expert": lax.rem(e + j, g)} for j in range(1, g)]
        + [{"tensor": 1 - t}]
    )
    put = pltpu.make_async_copy(coef, w.at[d, e], own.at[1])
    put.start()
    sends = []
    for k in range(1, n):
        to = lax.rem(d + k, n)
        for src, dst, a in ((columns(to, True), x.at[d, e, :, lanes], 0), (coef, w.at[d, e], 1)):
            copy = remote(src, dst, s1.at[a, k], r1.at[a, k], {"dp": to})
            copy.start()
            sends.append(copy)

    def view(a, block, peer):
        return x.at[block, peer, :, lanes] if a == 0 else w.at[block, peer]

    def cross(k, j, block, peer):
        at = x.at[block, peer, :, lanes]
        return remote(at, at, s3.at[k, j], r3.at[k, j], {"tensor": 1 - t})

    for k in range(n):
        block = lax.rem(d - k + n, n)
        for a in (0, 1):
            if k == 0:
                (mine, put)[a].wait()
            else:
                at = view(a, block, e)
                remote(at, at, s1.at[a, k], r1.at[a, k], {"dp": d}).wait_recv()
            for j in range(1, g):
                at = view(a, block, e)
                copy = remote(at, at, s2.at[a, k, j], r2.at[a, k, j], {"expert": lax.rem(e + j, g)})
                copy.start()
                sends.append(copy)
        if split and k:
            copy = cross(k, 0, block, e)
            copy.start()
            sends.append(copy)
    for k in range(n):
        block = lax.rem(d - k + n, n)
        for a in (0, 1):
            for j in range(1, g):
                peer = lax.rem(e - j + g, g)
                at = view(a, block, peer)
                remote(at, at, s2.at[a, k, j], r2.at[a, k, j], {"expert": e}).wait_recv()
                if a == 0 and split:
                    copy = cross(k, j, block, peer)
                    copy.start()
                    sends.append(copy)
    if split:
        other = pl.ds(pl.multiple_of((1 - t) * half, 128), half)
        for k in range(n):
            block = lax.rem(d - k + n, n)
            for j in range(g):
                if k or j:
                    at = x.at[block, lax.rem(e - j + g, g), :, other]
                    remote(at, at, s3.at[k, j], r3.at[k, j], {"tensor": t}).wait_recv()
    for copy in sends:
        copy.wait_send()


def dispatch(tokens, ids, weights, experts, n, g):
    rows, model = tokens.shape
    return pl.pallas_call(
        functools.partial(dispatch_kernel, n, g),
        out_shape=(
            jax.ShapeDtypeStruct((n, g, rows, model // n), tokens.dtype),
            jax.ShapeDtypeStruct((n, g, rows, experts), F32),
        ),
        in_specs=[VMEM] * 3,
        out_specs=(VMEM, VMEM),
        scratch_shapes=[
            pltpu.VMEM((rows, experts), F32),
            DMA((2,)), DMA((2, n)), DMA((2, n)), DMA((2, n, g)), DMA((2, n, g)),
            DMA((n, g)), DMA((n, g)),
        ],
        compiler_params=params(0),
    )(tokens, ids, weights)


def layer_kernel(
    n, g, sliced, x, w, gate, up, down, sgate, sup, sdown, y,
    xs, ws, gbuf, ubuf, dbuf, sgbuf, subuf, sdbuf, picked, compact, spread, sspread, acc, factor,
    own, got, out, hid, sown, sgot, sout, shid, here, there,
    wsem, dsem, ssem, s1, r1, s2, r2, t1, q1, t2, q2,
):
    d, e = lax.axis_index("dp"), lax.axis_index("expert")
    rows, width = x.shape[2:]
    experts = w.shape[3]
    local, hidden = gate.shape[0], gate.shape[2]
    thin = sgbuf.shape[1]
    wire = out.dtype
    tiles = xs.shape[0] // TILE
    slots = TILE // PITCH * CAP
    solid = TILE // PITCH * rows
    pairs = hidden // COLS // 2
    pieces = own.shape[1]
    blocks = local * pairs
    per = pieces // blocks
    prev, after = lax.rem(d - 1 + n, n), lax.rem(d + 1, n)
    place = (d, n - 1 - d)
    ahead = (jnp.minimum(d + 1, n - 1), jnp.maximum(d - 1, 0))
    behind = (jnp.maximum(d - 1, 0), jnp.minimum(d + 1, n - 1))

    def cut(c):
        return pl.ds(pl.multiple_of(c * COLS, COLS), COLS)

    def load(b):
        at = b // pairs
        wide = pl.ds(pl.multiple_of(lax.rem(b, pairs) * 2 * COLS, 2 * COLS), 2 * COLS)
        return [
            pltpu.make_async_copy(src.at[at, :, wide], dst.at[at, :, wide], wsem.at[h, b])
            for h, (src, dst) in enumerate(((gate, gbuf), (up, ubuf)))
        ]

    start = 0 if sliced else e * thin
    across = pl.ds(0, thin) if sliced else pl.ds(pl.multiple_of(start, thin), thin)
    extra = [
        pltpu.make_async_copy(sgate.at[:, across], sgbuf, ssem.at[0]),
        pltpu.make_async_copy(sup.at[:, across], subuf, ssem.at[1]),
        pltpu.make_async_copy(sdown.at[across, :], sdbuf, ssem.at[2]),
    ]
    lowers = [pltpu.make_async_copy(down.at[l], dbuf.at[l], dsem.at[l]) for l in range(local)]

    for copy in extra[:2]:
        copy.start()
    for b in range(min(AHEAD, blocks)):
        for copy in load(b):
            copy.start()

    greeted = pltpu.get_barrier_semaphore()
    for peer in (prev, after):
        pl.semaphore_signal(greeted, inc=1, device_id={"dp": peer}, device_id_type=MESH)

    xs[...] = jnp.zeros_like(xs)
    ws[...] = jnp.zeros_like(ws)
    for i in range(n):
        for j in range(g):
            at = (i * g + j) * PITCH
            xs[at:at + rows, :] = x[i, j]
            ws[at:at + rows, :] = w[i, j]

    def iota(shape, axis):
        return lax.broadcasted_iota(jnp.int32, shape, axis)

    token_row, token_col = iota((TILE, TILE), 0), iota((TILE, TILE), 1)
    same = token_row // PITCH == token_col // PITCH
    before = jnp.where(same & (token_row < token_col), 1.0, 0.0).astype(BF16)
    behind_in = jnp.where(same & (token_col < token_row), 1.0, 0.0).astype(BF16)
    spots = 16
    pick_rows = jnp.where(
        iota((spots, experts), 1) == e * local + iota((spots, experts), 0), 1.0, 0.0
    ).astype(BF16)
    base_row = iota((spots, TILE), 1) // PITCH * CAP
    base_col = iota((TILE, experts), 0) // PITCH * CAP
    for a in range(tiles):
        part = ws[a * TILE:(a + 1) * TILE, :]
        chosen = jnp.where(part > 0.0, 1.0, 0.0).astype(BF16)
        row = lax.dot_general(
            pick_rows, chosen, (((1,), (1,)), ((), ())), preferred_element_type=F32
        )
        rank_row = dot(row.astype(BF16), before).astype(jnp.int32)
        goal_row = jnp.where(row > 0.5, base_row + rank_row, -1)
        rank_col = dot(behind_in, chosen).astype(jnp.int32)
        goal_col = jnp.where(part > 0.0, base_col + rank_col, -1).astype(F32)
        for l in range(local):
            mark = iota((TILE, experts), 1) == e * local + l
            column = jnp.sum(jnp.where(mark, goal_col, 0.0), axis=1, keepdims=True)
            here[a, l] = jnp.where(
                goal_row[l:l + 1, :] == iota((slots, TILE), 0), 1.0, 0.0
            ).astype(BF16)
            there[a, l] = jnp.where(
                column.astype(jnp.int32) == iota((TILE, slots), 1), 1.0, 0.0
            ).astype(BF16)
            factor[l, a * TILE:(a + 1) * TILE, :] = jnp.sum(
                jnp.where(mark, part, 0.0), axis=1, keepdims=True
            )

    def solid_map(shape, slot_axis, token_axis):
        token, slot = iota(shape, token_axis), iota(shape, slot_axis)
        inside = token % PITCH
        return jnp.where(
            (inside < rows) & (token // PITCH * rows + inside == slot), 1.0, 0.0
        ).astype(BF16)

    rest = solid // 2
    pack_map = solid_map((solid, TILE), 0, 1)
    for a in range(tiles):
        compact[...] = dot(pack_map, xs[a * TILE:(a + 1) * TILE, :]).astype(BF16)
        if a == 0:
            for copy in extra[:2]:
                copy.wait()
        for h, buf in ((0, sgbuf), (1, subuf)):
            value = dot(compact[...], buf[...])
            for way in (0, 1):
                sown[way, 0, h, a * rest:(a + 1) * rest, :] = value[way * rest:(way + 1) * rest]

    pl.semaphore_wait(greeted, 2)

    routed = (own, got, out if wire == BF16 else own, hid, s1, r1, s2, r2)
    shared = (sown, sgot, sout if wire == BF16 else sown, shid, t1, q1, t2, q2)

    def partial_send(group, way, i):
        return remote(
            group[2].at[way, i], group[1].at[way, i], group[4].at[way, i], group[5].at[way, i],
            {"dp": ahead[way]},
        )

    def hidden_send(group, way, i):
        at = group[3].at[way, i]
        return remote(at, at, group[6].at[way, i], group[7].at[way, i], {"dp": behind[way]})

    def forward(group, way, i):
        mine, come, leave, final = group[:4]

        @pl.when(place[way] == 0)
        def _():
            if leave is not mine:
                for h in (0, 1):
                    leave[way, i, h] = packed(mine[way, i, h], wire)
            partial_send(group, way, i).start()

        @pl.when(place[way] > 0)
        def _():
            partial_send(group, way, i).wait_recv()

            @pl.when(place[way] < n - 1)
            def _():
                for h in (0, 1):
                    leave[way, i, h] = packed(mine[way, i, h] + unpacked(come[way, i, h]), wire)
                partial_send(group, way, i).start()

            @pl.when(place[way] == n - 1)
            def _():
                a, b = (mine[way, i, h] + unpacked(come[way, i, h]) for h in (0, 1))
                final[way, i] = (a / (1.0 + jnp.exp(-a)) * b).astype(final.dtype)
                hidden_send(group, way, i).start()

    def pass_on(group, way, i):
        hidden_send(group, way, i).wait_recv()

        @pl.when(place[way] > 0)
        def _():
            hidden_send(group, way, i).start()

    def project(b):
        at, c = b // pairs, lax.rem(b, pairs) * 2

        @pl.when(c == 0)
        def _():
            for a in range(tiles):
                picked[a] = dot(here[a, at], xs[a * TILE:(a + 1) * TILE, :]).astype(BF16)

        for copy in load(b):
            copy.wait()

        @pl.when(b + AHEAD < blocks)
        def _():
            for copy in load(b + AHEAD):
                copy.start()

        @pl.when(b + AHEAD == blocks)
        def _():
            for copy in extra[2:] + lowers:
                copy.start()

        fine = slots // ROWS
        for way in (0, 1):
            for h, buf in ((0, gbuf), (1, ubuf)):
                for a in range(tiles):
                    value = dot(picked[a], buf[at, :, cut(c + way)])
                    for r in range(fine):
                        own[way, b * per + a * fine + r, h] = value[r * ROWS:(r + 1) * ROWS]

    def stage(b, carry):
        @pl.when(b < blocks)
        def _():
            project(b)

        for r in range(per):
            s = b * per + r
            for way in (0, 1):
                @pl.when(s == SKEW * place[way])
                def _():
                    forward(shared, way, 0)

                i = s - SKEW * place[way]

                @pl.when((i >= 0) & (i < pieces))
                def _():
                    forward(routed, way, i)
        return carry

    lax.fori_loop(0, blocks + -(-SKEW * (n - 1) // per), stage, 0)

    part_of = TILE if width % TILE == 0 else 128
    chunks = width // part_of
    ready = []

    def gather(l):
        for way in (0, 1):
            for c in range(pairs):
                b = l * pairs + c
                fine = slots // ROWS
                for a in range(tiles):
                    value = hid[way, b * per + a * fine:b * per + (a + 1) * fine]
                    spread[a * TILE:(a + 1) * TILE, (2 * c + way) * COLS:(2 * c + way + 1) * COLS] = dot(
                        there[a, l], value.reshape(slots, COLS)
                    ).astype(BF16)

    def shared_gather():
        unpack_map = solid_map((TILE, solid), 1, 0)
        for a in range(tiles):
            value = jnp.concatenate([shid[way, 0, a * rest:(a + 1) * rest] for way in (0, 1)], axis=0)
            sspread[a * TILE:(a + 1) * TILE, :] = dot(unpack_map, value).astype(BF16)

    def shared_down(c):
        at = slice(c * part_of, (c + 1) * part_of)
        for a in range(tiles):
            span = slice(a * TILE, (a + 1) * TILE)
            acc[span, at] = dot(sspread[span, :], sdbuf[:, at])

    def routed_down(l, c):
        at = slice(c * part_of, (c + 1) * part_of)
        for a in range(tiles):
            span = slice(a * TILE, (a + 1) * TILE)
            acc[span, at] += factor[l, span, :] * dot(spread[span, :], dbuf[l, :, at])

    def flush(c):
        at = slice(c * part_of, (c + 1) * part_of)
        for i in range(n):
            for j in range(g):
                top = (i * g + j) * PITCH
                y[i, j, :, at] = acc[top:top + rows, at]

    lag = SPREAD_SKEW * (n - 2)
    each = pieces // local
    for s in range(pieces + lag):
        for way in (0, 1):
            late = n - 2 - place[way]

            @pl.when((late >= 0) & (s == SPREAD_SKEW * late))
            def _():
                pass_on(shared, way, 0)

            i = s - SPREAD_SKEW * late

            @pl.when((late >= 0) & (i >= 0) & (i < pieces))
            def _():
                pass_on(routed, way, i)
        if s == lag:
            def _start():
                extra[2].wait()
                shared_gather()
            ready.append(_start)
            ready += [functools.partial(shared_down, c) for c in range(chunks)]
        if s >= lag and (s - lag + 1) % each == 0:
            l = (s - lag + 1) // each - 1

            def _begin(l=l):
                lowers[l].wait()
                gather(l)
            ready.append(_begin)
            for c in range(chunks):
                ready.append(functools.partial(routed_down, l, c))
                if l == local - 1:
                    ready.append(functools.partial(flush, c))
        quota = 3 if s < pieces + lag - 1 else len(ready)
        for task in ready[:quota]:
            task()
        ready = ready[quota:]

    def finish(group, way, i):
        @pl.when(place[way] < n - 1)
        def _():
            partial_send(group, way, i).wait_send()

        @pl.when(place[way] > 0)
        def _():
            hidden_send(group, way, i).wait_send()

    def drain(i, carry):
        for way in (0, 1):
            finish(routed, way, i)
        return carry

    lax.fori_loop(0, pieces, drain, 0)
    for way in (0, 1):
        finish(shared, way, 0)


def layer(x, w, gate, up, down, sgate, sup, sdown, n, g):
    rows, width = x.shape[2:]
    experts = w.shape[3]
    local, _, hidden = gate.shape
    thin = hidden // g
    wire = BF16 if n <= 4 else F32
    sliced = thin % 128 != 0
    if sliced:
        e = lax.axis_index("expert")
        sgate = lax.dynamic_slice_in_dim(sgate, e * thin, thin, 1)
        sup = lax.dynamic_slice_in_dim(sup, e * thin, thin, 1)
        sdown = lax.dynamic_slice_in_dim(sdown, e * thin, thin, 0)
    count = n * g * PITCH
    tiles = count // TILE
    slots = TILE // PITCH * CAP
    blocks = local * (hidden // COLS // 2)
    pieces = blocks * tiles * (slots // ROWS)
    half = n * g * rows // 2
    return pl.pallas_call(
        functools.partial(layer_kernel, n, g, sliced),
        out_shape=jax.ShapeDtypeStruct((n, g, rows, width), F32),
        in_specs=[VMEM] * 2 + [HBM] * 6,
        out_specs=VMEM,
        scratch_shapes=[
            pltpu.VMEM((count, width), BF16),
            pltpu.VMEM((count, experts), F32),
            pltpu.VMEM((local, width, hidden), BF16),
            pltpu.VMEM((local, width, hidden), BF16),
            pltpu.VMEM((local, hidden, width), BF16),
            pltpu.VMEM((width, thin), BF16),
            pltpu.VMEM((width, thin), BF16),
            pltpu.VMEM((thin, width), BF16),
            pltpu.VMEM((tiles, slots, width), BF16),
            pltpu.VMEM((TILE // PITCH * rows, width), BF16),
            pltpu.VMEM((count, hidden), BF16),
            pltpu.VMEM((count, thin), BF16),
            pltpu.VMEM((count, width), F32),
            pltpu.VMEM((local, count, 1), F32),
            pltpu.VMEM((2, pieces, 2, ROWS, COLS), F32),
            pltpu.VMEM((2, pieces, 2, ROWS, COLS), wire),
            pltpu.VMEM((2, pieces, 2, ROWS, COLS) if wire == BF16 else (8, 128), wire),
            pltpu.VMEM((2, pieces, ROWS, COLS), BF16),
            pltpu.VMEM((2, 1, 2, half, thin), F32),
            pltpu.VMEM((2, 1, 2, half, thin), wire),
            pltpu.VMEM((2, 1, 2, half, thin), wire),
            pltpu.VMEM((2, 1, half, thin), BF16),
            pltpu.VMEM((tiles, local, slots, TILE), BF16),
            pltpu.VMEM((tiles, local, TILE, slots), BF16),
            DMA((2, blocks)), DMA((local,)), DMA((3,)),
            DMA((2, pieces)), DMA((2, pieces)), DMA((2, pieces)), DMA((2, pieces)),
            DMA((2, 1)), DMA((2, 1)), DMA((2, 1)), DMA((2, 1)),
        ],
        compiler_params=params(1, 67043328),
    )(x, w, gate, up, down, sgate, sup, sdown)


def collect_kernel(n, g, y, o, peer_in, z, ship, plane, done, sa, ra, sb, rb, sc, rc, own):
    d, e, t = lax.axis_index("dp"), lax.axis_index("expert"), lax.axis_index("tensor")
    other = 1 - t
    half = n // 2
    width = y.shape[3]

    def goal(block):
        return o.at[:, pl.ds(pl.multiple_of(block * width, 128), width)]

    greet(
        [{"tensor": other}]
        + [{"expert": lax.rem(e + j, g)} for j in range(1, g)]
        + [{"dp": lax.rem(d + k, n), "tensor": c} for k in range(1, n) for c in (0, 1)]
    )
    order = list(range(1, g)) + [0]
    swap = {}
    for j in order:
        to = lax.rem(e + j, g)
        swap[j] = remote(
            y.at[pl.ds(other * half, half), to], peer_in.at[to], sa.at[j], ra.at[j], {"tensor": other}
        )
        swap[j].start()
    sends = []
    for j in order:
        to = lax.rem(e + j, g)
        swap[j].wait_recv()
        total = y[pl.ds(t * half, half), to] + peer_in[to]
        if j:
            ship[j] = packed(total, ship.dtype)
            copy = remote(ship.at[j], plane.at[j], sb.at[j], rb.at[j], {"expert": to})
            copy.start()
            sends.append(copy)
        else:
            z[...] = total
    total = z[...]
    for j in range(1, g):
        sends[j - 1].wait_recv()
        total = total + unpacked(plane[j])
    done[...] = total.astype(done.dtype)
    last = []
    for i in range(half):
        home = t * half + i
        for c in (0, 1):
            here = (home == d) & (t == c)
            away = remote(
                done.at[i], goal(d), sc.at[i, c], rc.at[d], {"dp": home, "tensor": c}
            )
            pl.when(jnp.logical_not(here))(away.start)
            local = pltpu.make_async_copy(done.at[i], goal(d), own)
            pl.when(here)(local.start)
            last.append((here, away, local))
    for k in range(n):
        local_arrives = (d // half == t) & (d == k)

        @pl.when(jnp.logical_not(local_arrives))
        def _():
            remote(done.at[0], goal(k), sc.at[0, 0], rc.at[k], {"dp": d}).wait_recv()

    for here, away, local in last:
        pl.when(jnp.logical_not(here))(away.wait_send)
        pl.when(here)(local.wait)
    for copy in list(swap.values()) + sends:
        copy.wait_send()


def collect(y, n, g):
    rows, width = y.shape[2:]
    half = n // 2
    wire = BF16 if n <= 4 else F32
    return pl.pallas_call(
        functools.partial(collect_kernel, n, g),
        out_shape=jax.ShapeDtypeStruct((rows, n * width), BF16),
        in_specs=[VMEM],
        out_specs=VMEM,
        scratch_shapes=[
            pltpu.VMEM((g, half, rows, width), F32),
            pltpu.VMEM((half, rows, width), F32),
            pltpu.VMEM((g, half, rows, width), wire),
            pltpu.VMEM((g, half, rows, width), wire),
            pltpu.VMEM((half, rows, width), BF16),
            DMA((g,)), DMA((g,)), DMA((g,)), DMA((g,)), DMA((half, 2)), DMA((n,)), DMA,
        ],
        compiler_params=params(2),
    )(y)


def per_device(
    tokens, expert_ids, route_weights, gate_weights, up_weights, down_weights,
    shared_gate, shared_up, shared_down,
):
    g, n = lax.axis_size("expert"), lax.axis_size("dp")
    experts = gate_weights.shape[0] * g
    x, w = dispatch(tokens, expert_ids, route_weights, experts, n, g)
    y = layer(
        x, w, gate_weights, up_weights, down_weights, shared_gate, shared_up, shared_down, n, g
    )
    return collect(y, n, g)


def solution(mesh):
    placed = (
        P(("dp", "expert"), None),
        P(("dp", "expert"), None),
        P(("dp", "expert"), None),
        P("expert", "dp", "tensor"),
        P("expert", "dp", "tensor"),
        P("expert", "tensor", "dp"),
        P("dp", "tensor"),
        P("dp", "tensor"),
        P("tensor", "dp"),
    )
    return jax.shard_map(
        per_device, mesh=mesh, in_specs=placed, out_specs=P(("dp", "expert"), None), check_vma=False
    )
```

```python
import functools

import jax
import jax.numpy as jnp
from jax import lax
from jax.experimental import pallas as pl
from jax.experimental.pallas import tpu as pltpu
from jax.sharding import PartitionSpec as P

CAP = 8
PITCH = 16
TILE = 256
COLS = 256
ROWS = 64
AHEAD = 3
SKEW = 4
SPREAD_SKEW = 5
MESH = pl.DeviceIdType.MESH
VMEM = pl.BlockSpec(memory_space=pltpu.VMEM)
HBM = pl.BlockSpec(memory_space=pl.ANY)
DMA = pltpu.SemaphoreType.DMA
F32 = jnp.float32
BF16 = jnp.bfloat16


def greet(peers):
    barrier = pltpu.get_barrier_semaphore()
    for peer in peers:
        pl.semaphore_signal(barrier, inc=1, device_id=peer, device_id_type=MESH)
    pl.semaphore_wait(barrier, len(peers))


def remote(src, dst, send, recv, peer):
    return pltpu.make_async_remote_copy(
        src_ref=src, dst_ref=dst, send_sem=send, recv_sem=recv, device_id=peer, device_id_type=MESH
    )


def params(number, limit=60 * 1024 * 1024):
    return pltpu.CompilerParams(
        collective_id=number, has_side_effects=True, vmem_limit_bytes=limit
    )


def packed(v, wire):
    return v if wire == F32 else (v * jnp.abs(v)).astype(wire)


def unpacked(v):
    if v.dtype == F32:
        return v
    v = v.astype(F32)
    size = jnp.abs(v)
    root = size * lax.rsqrt(jnp.maximum(size, 1e-30))
    return jnp.where(v < 0.0, -root, root)


def dot(a, b):
    return jnp.dot(a, b, preferred_element_type=F32)


def dispatch_kernel(n, g, tok, ids, weights, x, w, coef, own, s1, r1, s2, r2, s3, r3):
    d, e, t = lax.axis_index("dp"), lax.axis_index("expert"), lax.axis_index("tensor")
    width, experts = x.shape[3], w.shape[3]
    split = (width // 2) % 128 == 0
    half = width // 2 if split else width
    lanes = pl.ds(pl.multiple_of(t * half, 128), half) if split else pl.ds(0, width)

    def columns(block, part):
        start = block * width + (t * half if part and split else 0)
        return tok.at[:, pl.ds(pl.multiple_of(start, 128), half if part else width)]

    mine = pltpu.make_async_copy(columns(d, False), x.at[d, e], own.at[0])
    mine.start()
    name = lax.broadcasted_iota(jnp.int32, coef.shape, 1)
    total = jnp.zeros(coef.shape, F32)
    for k in range(ids.shape[1]):
        total = total + jnp.where(ids[:, k:k + 1] == name, weights[:, k:k + 1], 0.0)
    coef[...] = total
    greet(
        [{"dp": lax.rem(d + k, n)} for k in range(1, n)]
        + [{"expert": lax.rem(e + j, g)} for j in range(1, g)]
        + [{"tensor": 1 - t}]
    )
    put = pltpu.make_async_copy(coef, w.at[d, e], own.at[1])
    put.start()
    sends = []
    for k in range(1, n):
        to = lax.rem(d + k, n)
        for src, dst, a in ((columns(to, True), x.at[d, e, :, lanes], 0), (coef, w.at[d, e], 1)):
            copy = remote(src, dst, s1.at[a, k], r1.at[a, k], {"dp": to})
            copy.start()
            sends.append(copy)

    def view(a, block, peer):
        return x.at[block, peer, :, lanes] if a == 0 else w.at[block, peer]

    def cross(k, j, block, peer):
        at = x.at[block, peer, :, lanes]
        return remote(at, at, s3.at[k, j], r3.at[k, j], {"tensor": 1 - t})

    for k in range(n):
        block = lax.rem(d - k + n, n)
        for a in (0, 1):
            if k == 0:
                (mine, put)[a].wait()
            else:
                at = view(a, block, e)
                remote(at, at, s1.at[a, k], r1.at[a, k], {"dp": d}).wait_recv()
            for j in range(1, g):
                at = view(a, block, e)
                copy = remote(at, at, s2.at[a, k, j], r2.at[a, k, j], {"expert": lax.rem(e + j, g)})
                copy.start()
                sends.append(copy)
        if split and k:
            copy = cross(k, 0, block, e)
            copy.start()
            sends.append(copy)
    for k in range(n):
        block = lax.rem(d - k + n, n)
        for a in (0, 1):
            for j in range(1, g):
                peer = lax.rem(e - j + g, g)
                at = view(a, block, peer)
                remote(at, at, s2.at[a, k, j], r2.at[a, k, j], {"expert": e}).wait_recv()
                if a == 0 and split:
                    copy = cross(k, j, block, peer)
                    copy.start()
                    sends.append(copy)
    if split:
        other = pl.ds(pl.multiple_of((1 - t) * half, 128), half)
        for k in range(n):
            block = lax.rem(d - k + n, n)
            for j in range(g):
                if k or j:
                    at = x.at[block, lax.rem(e - j + g, g), :, other]
                    remote(at, at, s3.at[k, j], r3.at[k, j], {"tensor": t}).wait_recv()
    for copy in sends:
        copy.wait_send()


def dispatch(tokens, ids, weights, experts, n, g):
    rows, model = tokens.shape
    return pl.pallas_call(
        functools.partial(dispatch_kernel, n, g),
        out_shape=(
            jax.ShapeDtypeStruct((n, g, rows, model // n), tokens.dtype),
            jax.ShapeDtypeStruct((n, g, rows, experts), F32),
        ),
        in_specs=[VMEM] * 3,
        out_specs=(VMEM, VMEM),
        scratch_shapes=[
            pltpu.VMEM((rows, experts), F32),
            DMA((2,)), DMA((2, n)), DMA((2, n)), DMA((2, n, g)), DMA((2, n, g)),
            DMA((n, g)), DMA((n, g)),
        ],
        compiler_params=params(0),
    )(tokens, ids, weights)


def layer_kernel(
    n, g, sliced, x, w, gate, up, down, sgate, sup, sdown, y,
    xs, ws, gbuf, ubuf, dbuf, sgbuf, subuf, sdbuf, picked, compact, spread, sspread, acc, factor,
    own, got, out, hid, sown, sgot, sout, shid, here, there,
    wsem, dsem, ssem, s1, r1, s2, r2, t1, q1, t2, q2,
):
    d, e = lax.axis_index("dp"), lax.axis_index("expert")
    rows, width = x.shape[2:]
    experts = w.shape[3]
    local, hidden = gate.shape[0], gate.shape[2]
    thin = sgbuf.shape[1]
    wire = out.dtype
    tiles = xs.shape[0] // TILE
    slots = TILE // PITCH * CAP
    solid = TILE // PITCH * rows
    pairs = hidden // COLS // 2
    pieces = own.shape[1]
    blocks = local * pairs
    per = pieces // blocks
    prev, after = lax.rem(d - 1 + n, n), lax.rem(d + 1, n)
    place = (d, n - 1 - d)
    ahead = (jnp.minimum(d + 1, n - 1), jnp.maximum(d - 1, 0))
    behind = (jnp.maximum(d - 1, 0), jnp.minimum(d + 1, n - 1))

    def cut(c):
        return pl.ds(pl.multiple_of(c * COLS, COLS), COLS)

    def load(b):
        at = b // pairs
        wide = pl.ds(pl.multiple_of(lax.rem(b, pairs) * 2 * COLS, 2 * COLS), 2 * COLS)
        return [
            pltpu.make_async_copy(src.at[at, :, wide], dst.at[at, :, wide], wsem.at[h, b])
            for h, (src, dst) in enumerate(((gate, gbuf), (up, ubuf)))
        ]

    start = 0 if sliced else e * thin
    across = pl.ds(0, thin) if sliced else pl.ds(pl.multiple_of(start, thin), thin)
    extra = [
        pltpu.make_async_copy(sgate.at[:, across], sgbuf, ssem.at[0]),
        pltpu.make_async_copy(sup.at[:, across], subuf, ssem.at[1]),
        pltpu.make_async_copy(sdown.at[across, :], sdbuf, ssem.at[2]),
    ]
    lowers = [pltpu.make_async_copy(down.at[l], dbuf.at[l], dsem.at[l]) for l in range(local)]

    for copy in extra[:2]:
        copy.start()
    for b in range(min(AHEAD, blocks)):
        for copy in load(b):
            copy.start()

    greeted = pltpu.get_barrier_semaphore()
    for peer in (prev, after):
        pl.semaphore_signal(greeted, inc=1, device_id={"dp": peer}, device_id_type=MESH)

    xs[...] = jnp.zeros_like(xs)
    ws[...] = jnp.zeros_like(ws)
    for i in range(n):
        for j in range(g):
            at = (i * g + j) * PITCH
            xs[at:at + rows, :] = x[i, j]
            ws[at:at + rows, :] = w[i, j]

    def iota(shape, axis):
        return lax.broadcasted_iota(jnp.int32, shape, axis)

    token_row, token_col = iota((TILE, TILE), 0), iota((TILE, TILE), 1)
    same = token_row // PITCH == token_col // PITCH
    before = jnp.where(same & (token_row < token_col), 1.0, 0.0).astype(BF16)
    behind_in = jnp.where(same & (token_col < token_row), 1.0, 0.0).astype(BF16)
    spots = 16
    pick_rows = jnp.where(
        iota((spots, experts), 1) == e * local + iota((spots, experts), 0), 1.0, 0.0
    ).astype(BF16)
    base_row = iota((spots, TILE), 1) // PITCH * CAP
    base_col = iota((TILE, experts), 0) // PITCH * CAP
    for a in range(tiles):
        part = ws[a * TILE:(a + 1) * TILE, :]
        chosen = jnp.where(part > 0.0, 1.0, 0.0).astype(BF16)
        row = lax.dot_general(
            pick_rows, chosen, (((1,), (1,)), ((), ())), preferred_element_type=F32
        )
        rank_row = dot(row.astype(BF16), before).astype(jnp.int32)
        goal_row = jnp.where(row > 0.5, base_row + rank_row, -1)
        rank_col = dot(behind_in, chosen).astype(jnp.int32)
        goal_col = jnp.where(part > 0.0, base_col + rank_col, -1).astype(F32)
        for l in range(local):
            mark = iota((TILE, experts), 1) == e * local + l
            column = jnp.sum(jnp.where(mark, goal_col, 0.0), axis=1, keepdims=True)
            here[a, l] = jnp.where(
                goal_row[l:l + 1, :] == iota((slots, TILE), 0), 1.0, 0.0
            ).astype(BF16)
            there[a, l] = jnp.where(
                column.astype(jnp.int32) == iota((TILE, slots), 1), 1.0, 0.0
            ).astype(BF16)
            factor[l, a * TILE:(a + 1) * TILE, :] = jnp.sum(
                jnp.where(mark, part, 0.0), axis=1, keepdims=True
            )

    def solid_map(shape, slot_axis, token_axis):
        token, slot = iota(shape, token_axis), iota(shape, slot_axis)
        inside = token % PITCH
        return jnp.where(
            (inside < rows) & (token // PITCH * rows + inside == slot), 1.0, 0.0
        ).astype(BF16)

    rest = solid // 2
    pack_map = solid_map((solid, TILE), 0, 1)
    for a in range(tiles):
        compact[...] = dot(pack_map, xs[a * TILE:(a + 1) * TILE, :]).astype(BF16)
        if a == 0:
            for copy in extra[:2]:
                copy.wait()
        for h, buf in ((0, sgbuf), (1, subuf)):
            value = dot(compact[...], buf[...])
            for way in (0, 1):
                sown[way, 0, h, a * rest:(a + 1) * rest, :] = value[way * rest:(way + 1) * rest]

    pl.semaphore_wait(greeted, 2)

    routed = (own, got, out if wire == BF16 else own, hid, s1, r1, s2, r2)
    shared = (sown, sgot, sout if wire == BF16 else sown, shid, t1, q1, t2, q2)

    def partial_send(group, way, i):
        return remote(
            group[2].at[way, i], group[1].at[way, i], group[4].at[way, i], group[5].at[way, i],
            {"dp": ahead[way]},
        )

    def hidden_send(group, way, i):
        at = group[3].at[way, i]
        return remote(at, at, group[6].at[way, i], group[7].at[way, i], {"dp": behind[way]})

    def forward(group, way, i):
        mine, come, leave, final = group[:4]

        @pl.when(place[way] == 0)
        def _():
            if leave is not mine:
                for h in (0, 1):
                    leave[way, i, h] = packed(mine[way, i, h], wire)
            partial_send(group, way, i).start()

        @pl.when(place[way] > 0)
        def _():
            partial_send(group, way, i).wait_recv()

            @pl.when(place[way] < n - 1)
            def _():
                for h in (0, 1):
                    leave[way, i, h] = packed(mine[way, i, h] + unpacked(come[way, i, h]), wire)
                partial_send(group, way, i).start()

            @pl.when(place[way] == n - 1)
            def _():
                a, b = (mine[way, i, h] + unpacked(come[way, i, h]) for h in (0, 1))
                final[way, i] = (a / (1.0 + jnp.exp(-a)) * b).astype(final.dtype)
                hidden_send(group, way, i).start()

    def pass_on(group, way, i):
        hidden_send(group, way, i).wait_recv()

        @pl.when(place[way] > 0)
        def _():
            hidden_send(group, way, i).start()

    def project(b):
        at, c = b // pairs, lax.rem(b, pairs) * 2

        @pl.when(c == 0)
        def _():
            for a in range(tiles):
                picked[a] = dot(here[a, at], xs[a * TILE:(a + 1) * TILE, :]).astype(BF16)

        for copy in load(b):
            copy.wait()

        @pl.when(b + AHEAD < blocks)
        def _():
            for copy in load(b + AHEAD):
                copy.start()

        @pl.when(b + AHEAD == blocks)
        def _():
            for copy in extra[2:] + lowers:
                copy.start()

        fine = slots // ROWS
        for way in (0, 1):
            for h, buf in ((0, gbuf), (1, ubuf)):
                for a in range(tiles):
                    value = dot(picked[a], buf[at, :, cut(c + way)])
                    for r in range(fine):
                        own[way, b * per + a * fine + r, h] = value[r * ROWS:(r + 1) * ROWS]

    def stage(b, carry):
        @pl.when(b < blocks)
        def _():
            project(b)

        for r in range(per):
            s = b * per + r
            for way in (0, 1):
                @pl.when(s == SKEW * place[way])
                def _():
                    forward(shared, way, 0)

                i = s - SKEW * place[way]

                @pl.when((i >= 0) & (i < pieces))
                def _():
                    forward(routed, way, i)
        return carry

    lax.fori_loop(0, blocks + -(-SKEW * (n - 1) // per), stage, 0)

    part_of = TILE if width % TILE == 0 else 128
    chunks = width // part_of
    ready = []

    def gather(l):
        for way in (0, 1):
            for c in range(pairs):
                b = l * pairs + c
                fine = slots // ROWS
                for a in range(tiles):
                    value = hid[way, b * per + a * fine:b * per + (a + 1) * fine]
                    spread[a * TILE:(a + 1) * TILE, (2 * c + way) * COLS:(2 * c + way + 1) * COLS] = dot(
                        there[a, l], value.reshape(slots, COLS)
                    ).astype(BF16)

    def shared_gather():
        unpack_map = solid_map((TILE, solid), 1, 0)
        for a in range(tiles):
            value = jnp.concatenate([shid[way, 0, a * rest:(a + 1) * rest] for way in (0, 1)], axis=0)
            sspread[a * TILE:(a + 1) * TILE, :] = dot(unpack_map, value).astype(BF16)

    def shared_down(c):
        at = slice(c * part_of, (c + 1) * part_of)
        for a in range(tiles):
            span = slice(a * TILE, (a + 1) * TILE)
            acc[span, at] = dot(sspread[span, :], sdbuf[:, at])

    def routed_down(l, c):
        at = slice(c * part_of, (c + 1) * part_of)
        for a in range(tiles):
            span = slice(a * TILE, (a + 1) * TILE)
            acc[span, at] += factor[l, span, :] * dot(spread[span, :], dbuf[l, :, at])

    def flush(c):
        at = slice(c * part_of, (c + 1) * part_of)
        for i in range(n):
            for j in range(g):
                top = (i * g + j) * PITCH
                y[i, j, :, at] = acc[top:top + rows, at]

    lag = SPREAD_SKEW * (n - 2)
    each = pieces // local
    for s in range(pieces + lag):
        for way in (0, 1):
            late = n - 2 - place[way]

            @pl.when((late >= 0) & (s == SPREAD_SKEW * late))
            def _():
                pass_on(shared, way, 0)

            i = s - SPREAD_SKEW * late

            @pl.when((late >= 0) & (i >= 0) & (i < pieces))
            def _():
                pass_on(routed, way, i)
        if s == lag:
            def _start():
                extra[2].wait()
                shared_gather()
            ready.append(_start)
            ready += [functools.partial(shared_down, c) for c in range(chunks)]
        if s >= lag and (s - lag + 1) % each == 0:
            l = (s - lag + 1) // each - 1

            def _begin(l=l):
                lowers[l].wait()
                gather(l)
            ready.append(_begin)
            for c in range(chunks):
                ready.append(functools.partial(routed_down, l, c))
                if l == local - 1:
                    ready.append(functools.partial(flush, c))
        quota = 3 if s < pieces + lag - 1 else len(ready)
        for task in ready[:quota]:
            task()
        ready = ready[quota:]

    def finish(group, way, i):
        @pl.when(place[way] < n - 1)
        def _():
            partial_send(group, way, i).wait_send()

        @pl.when(place[way] > 0)
        def _():
            hidden_send(group, way, i).wait_send()

    def drain(i, carry):
        for way in (0, 1):
            finish(routed, way, i)
        return carry

    lax.fori_loop(0, pieces, drain, 0)
    for way in (0, 1):
        finish(shared, way, 0)


def layer(x, w, gate, up, down, sgate, sup, sdown, n, g):
    rows, width = x.shape[2:]
    experts = w.shape[3]
    local, _, hidden = gate.shape
    thin = hidden // g
    wire = BF16 if n <= 4 else F32
    sliced = thin % 128 != 0
    if sliced:
        e = lax.axis_index("expert")
        sgate = lax.dynamic_slice_in_dim(sgate, e * thin, thin, 1)
        sup = lax.dynamic_slice_in_dim(sup, e * thin, thin, 1)
        sdown = lax.dynamic_slice_in_dim(sdown, e * thin, thin, 0)
    count = n * g * PITCH
    tiles = count // TILE
    slots = TILE // PITCH * CAP
    blocks = local * (hidden // COLS // 2)
    pieces = blocks * tiles * (slots // ROWS)
    half = n * g * rows // 2
    return pl.pallas_call(
        functools.partial(layer_kernel, n, g, sliced),
        out_shape=jax.ShapeDtypeStruct((n, g, rows, width), F32),
        in_specs=[VMEM] * 2 + [HBM] * 6,
        out_specs=VMEM,
        scratch_shapes=[
            pltpu.VMEM((count, width), BF16),
            pltpu.VMEM((count, experts), F32),
            pltpu.VMEM((local, width, hidden), BF16),
            pltpu.VMEM((local, width, hidden), BF16),
            pltpu.VMEM((local, hidden, width), BF16),
            pltpu.VMEM((width, thin), BF16),
            pltpu.VMEM((width, thin), BF16),
            pltpu.VMEM((thin, width), BF16),
            pltpu.VMEM((tiles, slots, width), BF16),
            pltpu.VMEM((TILE // PITCH * rows, width), BF16),
            pltpu.VMEM((count, hidden), BF16),
            pltpu.VMEM((count, thin), BF16),
            pltpu.VMEM((count, width), F32),
            pltpu.VMEM((local, count, 1), F32),
            pltpu.VMEM((2, pieces, 2, ROWS, COLS), F32),
            pltpu.VMEM((2, pieces, 2, ROWS, COLS), wire),
            pltpu.VMEM((2, pieces, 2, ROWS, COLS) if wire == BF16 else (8, 128), wire),
            pltpu.VMEM((2, pieces, ROWS, COLS), BF16),
            pltpu.VMEM((2, 1, 2, half, thin), F32),
            pltpu.VMEM((2, 1, 2, half, thin), wire),
            pltpu.VMEM((2, 1, 2, half, thin), wire),
            pltpu.VMEM((2, 1, half, thin), BF16),
            pltpu.VMEM((tiles, local, slots, TILE), BF16),
            pltpu.VMEM((tiles, local, TILE, slots), BF16),
            DMA((2, blocks)), DMA((local,)), DMA((3,)),
            DMA((2, pieces)), DMA((2, pieces)), DMA((2, pieces)), DMA((2, pieces)),
            DMA((2, 1)), DMA((2, 1)), DMA((2, 1)), DMA((2, 1)),
        ],
        compiler_params=params(1, 67043328),
    )(x, w, gate, up, down, sgate, sup, sdown)


def collect_kernel(n, g, y, o, peer_in, z, ship, plane, done, sa, ra, sb, rb, sc, rc, own):
    d, e, t = lax.axis_index("dp"), lax.axis_index("expert"), lax.axis_index("tensor")
    other = 1 - t
    half = n // 2
    width = y.shape[3]

    def goal(block):
        return o.at[:, pl.ds(pl.multiple_of(block * width, 128), width)]

    greet(
        [{"tensor": other}]
        + [{"expert": lax.rem(e + j, g)} for j in range(1, g)]
        + [{"dp": lax.rem(d + k, n), "tensor": c} for k in range(1, n) for c in (0, 1)]
    )
    order = list(range(1, g)) + [0]
    swap = {}
    for j in order:
        to = lax.rem(e + j, g)
        swap[j] = remote(
            y.at[pl.ds(other * half, half), to], peer_in.at[to], sa.at[j], ra.at[j], {"tensor": other}
        )
        swap[j].start()
    sends = []
    for j in order:
        to = lax.rem(e + j, g)
        swap[j].wait_recv()
        total = y[pl.ds(t * half, half), to] + peer_in[to]
        if j:
            ship[j] = packed(total, ship.dtype)
            copy = remote(ship.at[j], plane.at[j], sb.at[j], rb.at[j], {"expert": to})
            copy.start()
            sends.append(copy)
        else:
            z[...] = total
    total = z[...]
    for j in range(1, g):
        sends[j - 1].wait_recv()
        total = total + unpacked(plane[j])
    done[...] = total.astype(done.dtype)
    last = []
    for i in range(half):
        home = t * half + i
        for c in (0, 1):
            here = (home == d) & (t == c)
            away = remote(
                done.at[i], goal(d), sc.at[i, c], rc.at[d], {"dp": home, "tensor": c}
            )
            pl.when(jnp.logical_not(here))(away.start)
            local = pltpu.make_async_copy(done.at[i], goal(d), own)
            pl.when(here)(local.start)
            last.append((here, away, local))
    for k in range(n):
        local_arrives = (d // half == t) & (d == k)

        @pl.when(jnp.logical_not(local_arrives))
        def _():
            remote(done.at[0], goal(k), sc.at[0, 0], rc.at[k], {"dp": d}).wait_recv()

    for here, away, local in last:
        pl.when(jnp.logical_not(here))(away.wait_send)
        pl.when(here)(local.wait)
    for copy in list(swap.values()) + sends:
        copy.wait_send()


def collect(y, n, g):
    rows, width = y.shape[2:]
    half = n // 2
    wire = BF16 if n <= 4 else F32
    return pl.pallas_call(
        functools.partial(collect_kernel, n, g),
        out_shape=jax.ShapeDtypeStruct((rows, n * width), BF16),
        in_specs=[VMEM],
        out_specs=VMEM,
        scratch_shapes=[
            pltpu.VMEM((g, half, rows, width), F32),
            pltpu.VMEM((half, rows, width), F32),
            pltpu.VMEM((g, half, rows, width), wire),
            pltpu.VMEM((g, half, rows, width), wire),
            pltpu.VMEM((half, rows, width), BF16),
            DMA((g,)), DMA((g,)), DMA((g,)), DMA((g,)), DMA((half, 2)), DMA((n,)), DMA,
        ],
        compiler_params=params(2),
    )(y)


def per_device(
    tokens, expert_ids, route_weights, gate_weights, up_weights, down_weights,
    shared_gate, shared_up, shared_down,
):
    g, n = lax.axis_size("expert"), lax.axis_size("dp")
    experts = gate_weights.shape[0] * g
    x, w = dispatch(tokens, expert_ids, route_weights, experts, n, g)
    y = layer(
        x, w, gate_weights, up_weights, down_weights, shared_gate, shared_up, shared_down, n, g
    )
    return collect(y, n, g)


def solution(mesh):
    placed = (
        P(("dp", "expert"), None),
        P(("dp", "expert"), None),
        P(("dp", "expert"), None),
        P("expert", "dp", "tensor"),
        P("expert", "dp", "tensor"),
        P("expert", "tensor", "dp"),
        P("dp", "tensor"),
        P("dp", "tensor"),
        P("tensor", "dp"),
    )
    return jax.shard_map(
        per_device, mesh=mesh, in_specs=placed, out_specs=P(("dp", "expert"), None), check_vma=False
    )
```

```python
import functools

import jax
import jax.numpy as jnp
from jax import lax
from jax.experimental import pallas as pl
from jax.experimental.pallas import tpu as pltpu
from jax.sharding import PartitionSpec as P

CAP = 8
PITCH = 16
TILE = 256
COLS = 256
ROWS = 64
AHEAD = 3
SKEW = 4
SPREAD_SKEW = 5
MESH = pl.DeviceIdType.MESH
VMEM = pl.BlockSpec(memory_space=pltpu.VMEM)
HBM = pl.BlockSpec(memory_space=pl.ANY)
DMA = pltpu.SemaphoreType.DMA
F32 = jnp.float32
BF16 = jnp.bfloat16


def greet(peers):
    barrier = pltpu.get_barrier_semaphore()
    for peer in peers:
        pl.semaphore_signal(barrier, inc=1, device_id=peer, device_id_type=MESH)
    pl.semaphore_wait(barrier, len(peers))


def remote(src, dst, send, recv, peer):
    return pltpu.make_async_remote_copy(
        src_ref=src, dst_ref=dst, send_sem=send, recv_sem=recv, device_id=peer, device_id_type=MESH
    )


def packed(v, wire):
    return v if wire == F32 else (v * jnp.abs(v)).astype(wire)


def unpacked(v):
    if v.dtype == F32:
        return v
    v = v.astype(F32)
    size = jnp.abs(v)
    root = size * lax.rsqrt(jnp.maximum(size, 1e-30))
    return jnp.where(v < 0.0, -root, root)


def dot(a, b):
    return jnp.dot(a, b, preferred_element_type=F32)


def layer_kernel(
    n, g, sliced, tok, ids, weights, gate, up, down, sgate, sup, sdown, o,
    x, w, coef, xs, ws, gbuf, ubuf, dbuf, sgbuf, subuf, sdbuf, picked, compact, spread, sspread, acc, factor,
    own, got, out, hid, sown, sgot, sout, shid, here, there, peer_in, kept, ship, plane, done,
    wsem, dsem, ssem, s1, r1, s2, r2, t1, q1, t2, q2,
    lsem, u1, v1, u2, v2, u3, v3, sa, ra, sb, rb, sc, rc, osem,
):
    d, e, t = lax.axis_index("dp"), lax.axis_index("expert"), lax.axis_index("tensor")
    other = 1 - t
    rows, width = x.shape[2:]
    experts = w.shape[3]
    local, hidden = gate.shape[0], gate.shape[2]
    thin = sgbuf.shape[1]
    wire = out.dtype
    tiles = xs.shape[0] // TILE
    slots = TILE // PITCH * CAP
    solid = TILE // PITCH * rows
    pairs = hidden // COLS // 2
    pieces = own.shape[1]
    blocks = local * pairs
    per = pieces // blocks
    place = (d, n - 1 - d)
    ahead = (jnp.minimum(d + 1, n - 1), jnp.maximum(d - 1, 0))
    behind = (jnp.maximum(d - 1, 0), jnp.minimum(d + 1, n - 1))

    def load(b):
        at, slot = b // pairs, lax.rem(b, gbuf.shape[0])
        wide = pl.ds(pl.multiple_of(lax.rem(b, pairs) * 2 * COLS, 2 * COLS), 2 * COLS)
        return [
            pltpu.make_async_copy(src.at[at, :, wide], dst.at[slot], wsem.at[h, b])
            for h, (src, dst) in enumerate(((gate, gbuf), (up, ubuf)))
        ]

    start = 0 if sliced else e * thin
    across = pl.ds(0, thin) if sliced else pl.ds(pl.multiple_of(start, thin), thin)
    extra = [
        pltpu.make_async_copy(sgate.at[:, across], sgbuf, ssem.at[0]),
        pltpu.make_async_copy(sup.at[:, across], subuf, ssem.at[1]),
        pltpu.make_async_copy(sdown.at[across, :], sdbuf, ssem.at[2]),
    ]
    lowers = [pltpu.make_async_copy(down.at[l], dbuf.at[l], dsem.at[l]) for l in range(local)]

    for copy in extra[:2]:
        copy.start()
    for b in range(min(AHEAD, blocks)):
        for copy in load(b):
            copy.start()

    split = (width // 2) % 128 == 0
    part_lanes = width // 2 if split else width
    lanes = pl.ds(pl.multiple_of(t * part_lanes, 128), part_lanes) if split else pl.ds(0, width)

    def columns(block, part):
        first = block * width + (t * part_lanes if part and split else 0)
        return tok.at[:, pl.ds(pl.multiple_of(first, 128), part_lanes if part else width)]

    mine = pltpu.make_async_copy(columns(d, False), x.at[d, e], lsem.at[0])
    mine.start()
    name = lax.broadcasted_iota(jnp.int32, coef.shape, 1)
    named, held = ids[...].T, weights[...].T
    total = jnp.zeros(coef.shape, F32)
    for k in range(ids.shape[0]):
        total = total + jnp.where(named[:, k:k + 1] == name, held[:, k:k + 1], 0.0)
    coef[...] = total
    greet(
        [{"tensor": other}]
        + [{"expert": lax.rem(e + j, g)} for j in range(1, g)]
        + [{"dp": lax.rem(d + k, n), "tensor": c} for k in range(1, n) for c in (0, 1)]
    )
    put = pltpu.make_async_copy(coef, w.at[d, e], lsem.at[1])
    put.start()
    sends = []
    for k in range(1, n):
        to = lax.rem(d + k, n)
        for src, dst, a in ((coef, w.at[d, e], 1), (columns(to, True), x.at[d, e, :, lanes], 0)):
            copy = remote(src, dst, u1.at[a, k], v1.at[a, k], {"dp": to})
            copy.start()
            sends.append(copy)

    def view(a, block, peer):
        return x.at[block, peer, :, lanes] if a == 0 else w.at[block, peer]

    def cross(k, j, block, peer):
        at = x.at[block, peer, :, lanes]
        return remote(at, at, u3.at[k, j], v3.at[k, j], {"tensor": other})

    xs[...] = jnp.zeros_like(xs)
    ws[...] = jnp.zeros_like(ws)
    for k in range(n):
        block = lax.rem(d - k + n, n)
        for a in (1, 0):
            if k == 0:
                (mine, put)[a].wait()
            else:
                at = view(a, block, e)
                remote(at, at, u1.at[a, k], v1.at[a, k], {"dp": d}).wait_recv()
            for j in range(1, g):
                at = view(a, block, e)
                copy = remote(at, at, u2.at[a, k, j], v2.at[a, k, j], {"expert": lax.rem(e + j, g)})
                copy.start()
                sends.append(copy)
        if split and k:
            copy = cross(k, 0, block, e)
            copy.start()
            sends.append(copy)

    def crossed(k, j, a):
        at = view(a, lax.rem(d - k + n, n), lax.rem(e - j + g, g))
        remote(at, at, u2.at[a, k, j], v2.at[a, k, j], {"expert": e}).wait_recv()

    for k in range(n):
        for j in range(1, g):
            crossed(k, j, 1)
    for i in range(n):
        for j in range(g):
            at = (i * g + j) * PITCH
            ws[at:at + rows, :] = w[i, j]

    def iota(shape, axis):
        return lax.broadcasted_iota(jnp.int32, shape, axis)

    token_row, token_col = iota((TILE, TILE), 0), iota((TILE, TILE), 1)
    same = token_row // PITCH == token_col // PITCH
    before = jnp.where(same & (token_row < token_col), 1.0, 0.0).astype(BF16)
    behind_in = jnp.where(same & (token_col < token_row), 1.0, 0.0).astype(BF16)
    spots = 16
    pick_rows = jnp.where(
        iota((spots, experts), 1) == e * local + iota((spots, experts), 0), 1.0, 0.0
    ).astype(BF16)
    base_row = iota((spots, TILE), 1) // PITCH * CAP
    base_col = iota((TILE, experts), 0) // PITCH * CAP
    for a in range(tiles):
        part = ws[a * TILE:(a + 1) * TILE, :]
        chosen = jnp.where(part > 0.0, 1.0, 0.0).astype(BF16)
        row = lax.dot_general(
            pick_rows, chosen, (((1,), (1,)), ((), ())), preferred_element_type=F32
        )
        rank_row = dot(row.astype(BF16), before).astype(jnp.int32)
        goal_row = jnp.where(row > 0.5, base_row + rank_row, -1)
        rank_col = dot(behind_in, chosen).astype(jnp.int32)
        goal_col = jnp.where(part > 0.0, base_col + rank_col, -1).astype(F32)
        for l in range(local):
            mark = iota((TILE, experts), 1) == e * local + l
            column = jnp.sum(jnp.where(mark, goal_col, 0.0), axis=1, keepdims=True)
            here[a, l] = jnp.where(
                goal_row[l:l + 1, :] == iota((slots, TILE), 0), 1.0, 0.0
            ).astype(BF16)
            there[a, l] = jnp.where(
                column.astype(jnp.int32) == iota((TILE, slots), 1), 1.0, 0.0
            ).astype(BF16)
            factor[l, a * TILE:(a + 1) * TILE, :] = jnp.sum(
                jnp.where(mark, part, 0.0), axis=1, keepdims=True
            )

    for k in range(n):
        for j in range(1, g):
            crossed(k, j, 0)
            if split:
                copy = cross(k, j, lax.rem(d - k + n, n), lax.rem(e - j + g, g))
                copy.start()
                sends.append(copy)
    if split:
        rest_lanes = pl.ds(pl.multiple_of(other * part_lanes, 128), part_lanes)
        for k in range(n):
            for j in range(g):
                if k or j:
                    at = x.at[lax.rem(d - k + n, n), lax.rem(e - j + g, g), :, rest_lanes]
                    remote(at, at, u3.at[k, j], v3.at[k, j], {"tensor": t}).wait_recv()
    for i in range(n):
        for j in range(g):
            at = (i * g + j) * PITCH
            xs[at:at + rows, :] = x[i, j]

    def solid_map(shape, slot_axis, token_axis):
        token, slot = iota(shape, token_axis), iota(shape, slot_axis)
        inside = token % PITCH
        return jnp.where(
            (inside < rows) & (token // PITCH * rows + inside == slot), 1.0, 0.0
        ).astype(BF16)

    rest = solid // 2
    pack_map = solid_map((solid, TILE), 0, 1)
    for a in range(tiles):
        compact[...] = dot(pack_map, xs[a * TILE:(a + 1) * TILE, :]).astype(BF16)
        if a == 0:
            for copy in extra[:2]:
                copy.wait()
        for h, buf in ((0, sgbuf), (1, subuf)):
            value = dot(compact[...], buf[...])
            for way in (0, 1):
                sown[way, 0, h, a * rest:(a + 1) * rest, :] = value[way * rest:(way + 1) * rest]

    routed = (own, got, out if wire == BF16 else own, hid, s1, r1, s2, r2)
    shared = (sown, sgot, sout if wire == BF16 else sown, shid, t1, q1, t2, q2)

    def partial_send(group, way, i):
        return remote(
            group[2].at[way, i], group[1].at[way, i], group[4].at[way, i], group[5].at[way, i],
            {"dp": ahead[way]},
        )

    def hidden_send(group, way, i):
        at = group[3].at[way, i]
        return remote(at, at, group[6].at[way, i], group[7].at[way, i], {"dp": behind[way]})

    def forward(group, way, i):
        mine, come, leave, final = group[:4]

        @pl.when(place[way] == 0)
        def _():
            if leave is not mine:
                for h in (0, 1):
                    leave[way, i, h] = packed(mine[way, i, h], wire)
            partial_send(group, way, i).start()

        @pl.when(place[way] > 0)
        def _():
            partial_send(group, way, i).wait_recv()

            @pl.when(place[way] < n - 1)
            def _():
                for h in (0, 1):
                    leave[way, i, h] = packed(mine[way, i, h] + unpacked(come[way, i, h]), wire)
                partial_send(group, way, i).start()

            @pl.when(place[way] == n - 1)
            def _():
                a, b = (mine[way, i, h] + unpacked(come[way, i, h]) for h in (0, 1))
                final[way, i] = (a / (1.0 + jnp.exp(-a)) * b).astype(final.dtype)
                hidden_send(group, way, i).start()

    def pass_on(group, way, i):
        hidden_send(group, way, i).wait_recv()

        @pl.when(place[way] > 0)
        def _():
            hidden_send(group, way, i).start()

    def project(b):
        at, slot = b // pairs, lax.rem(b, gbuf.shape[0])

        @pl.when(lax.rem(b, pairs) == 0)
        def _():
            for a in range(tiles):
                picked[a] = dot(here[a, at], xs[a * TILE:(a + 1) * TILE, :]).astype(BF16)

        for copy in load(b):
            copy.wait()

        @pl.when(b + AHEAD < blocks)
        def _():
            for copy in load(b + AHEAD):
                copy.start()

        @pl.when(b + AHEAD == blocks)
        def _():
            for copy in extra[2:] + lowers:
                copy.start()

        fine = slots // ROWS
        for way in (0, 1):
            for h, buf in ((0, gbuf), (1, ubuf)):
                for a in range(tiles):
                    value = dot(picked[a], buf[slot, :, way * COLS:(way + 1) * COLS])
                    for r in range(fine):
                        own[way, b * per + a * fine + r, h] = value[r * ROWS:(r + 1) * ROWS]

    def stage(b, carry):
        @pl.when(b < blocks)
        def _():
            project(b)

        for r in range(per):
            s = b * per + r
            for way in (0, 1):
                @pl.when(s == SKEW * place[way])
                def _():
                    forward(shared, way, 0)

                i = s - SKEW * place[way]

                @pl.when((i >= 0) & (i < pieces))
                def _():
                    forward(routed, way, i)
        return carry

    lax.fori_loop(0, blocks + -(-SKEW * (n - 1) // per), stage, 0)

    part_of = TILE if width % TILE == 0 else 128
    chunks = width // part_of
    ready = []

    def gather(l):
        for way in (0, 1):
            for c in range(pairs):
                b = l * pairs + c
                fine = slots // ROWS
                for a in range(tiles):
                    value = hid[way, b * per + a * fine:b * per + (a + 1) * fine]
                    spread[a * TILE:(a + 1) * TILE, (2 * c + way) * COLS:(2 * c + way + 1) * COLS] = dot(
                        there[a, l], value.reshape(slots, COLS)
                    ).astype(BF16)

    def shared_gather():
        unpack_map = solid_map((TILE, solid), 1, 0)
        for a in range(tiles):
            value = jnp.concatenate([shid[way, 0, a * rest:(a + 1) * rest] for way in (0, 1)], axis=0)
            sspread[a * TILE:(a + 1) * TILE, :] = dot(unpack_map, value).astype(BF16)

    deep = TILE // PITCH // g

    def shared_down(c):
        at = slice(c * part_of, (c + 1) * part_of)
        for a in range(tiles):
            span = slice(a * TILE, (a + 1) * TILE)
            value = dot(sspread[span, :], sdbuf[:, at])
            acc[a * deep:(a + 1) * deep, :, :, at] = value.reshape(deep, g, PITCH, part_of)

    def routed_down(l, c):
        at = slice(c * part_of, (c + 1) * part_of)
        for a in range(tiles):
            span = slice(a * TILE, (a + 1) * TILE)
            value = factor[l, span, :] * dot(spread[span, :], dbuf[l, :, at])
            acc[a * deep:(a + 1) * deep, :, :, at] += value.reshape(deep, g, PITCH, part_of)

    pool = n // 2
    cuts = [0, (chunks + 1) // 2, chunks]
    groups = [(cuts[q] * part_of, cuts[q + 1] * part_of) for q in (0, 1)]
    order = list(range(1, g)) + [0]

    def swap(q, j):
        lo, hi = groups[q]
        to = lax.rem(e + j, g)
        return remote(
            acc.at[pl.ds(other * pool, pool), to, :, pl.ds(lo, hi - lo)],
            peer_in.at[to, :, :, pl.ds(lo, hi - lo)], sa.at[q, j], ra.at[q, j], {"tensor": other},
        )

    def ship_to(q, j):
        lo, hi = groups[q]
        return remote(
            ship.at[j, :, :, pl.ds(lo, hi - lo)], plane.at[j, :, :, pl.ds(lo, hi - lo)],
            sb.at[q, j], rb.at[q, j], {"expert": lax.rem(e + j, g)},
        )

    def swap_out(q):
        for j in order:
            swap(q, j).start()

    def add_up(q):
        lo, hi = groups[q]
        for j in order:
            to = lax.rem(e + j, g)
            swap(q, j).wait_recv()
            value = acc[pl.ds(t * pool, pool), to, :, lo:hi] + peer_in[to, :, :, lo:hi]
            value = value[:, :rows]
            if j:
                ship[j, :, :, lo:hi] = packed(value, ship.dtype)
                ship_to(q, j).start()
            else:
                kept[:, :, lo:hi] = value

    def goal(q, block):
        lo, hi = groups[q]
        return o.at[:, pl.ds(pl.multiple_of(block * width + lo, 128), hi - lo)]

    def home_send(q, i):
        lo, hi = groups[q]
        home = t * pool + i
        src = done.at[i, :, pl.ds(lo, hi - lo)]
        copies = []
        for c in (0, 1):
            inside = (home == d) & (t == c)
            away = remote(src, goal(q, d), sc.at[q, i, c], rc.at[q, d], {"dp": home, "tensor": c})
            local_copy = pltpu.make_async_copy(src, goal(q, d), osem.at[q])
            copies.append((inside, away, local_copy))
        return copies

    def send_home(q):
        lo, hi = groups[q]
        value = kept[:, :, lo:hi]
        for j in range(1, g):
            ship_to(q, j).wait_recv()
            value = value + unpacked(plane[j, :, :, lo:hi])
        done[:, :, lo:hi] = value.astype(done.dtype)
        for i in range(pool):
            for inside, away, local_copy in home_send(q, i):
                pl.when(jnp.logical_not(inside))(away.start)
                pl.when(inside)(local_copy.start)

    def arrive(q):
        for k in range(n):
            stays = (d // pool == t) & (d == k)

            @pl.when(jnp.logical_not(stays))
            def _():
                lo, hi = groups[q]
                remote(
                    done.at[0, :, pl.ds(lo, hi - lo)], goal(q, k), sc.at[q, 0, 0], rc.at[q, k], {"dp": d}
                ).wait_recv()
        for i in range(pool):
            for inside, away, local_copy in home_send(q, i):
                pl.when(jnp.logical_not(inside))(away.wait_send)
                pl.when(inside)(local_copy.wait)
        for j in order:
            swap(q, j).wait_send()
            if j:
                ship_to(q, j).wait_send()

    lag = SPREAD_SKEW * (n - 2)
    each = pieces // local
    for s in range(pieces + lag):
        for way in (0, 1):
            late = n - 2 - place[way]

            @pl.when((late >= 0) & (s == SPREAD_SKEW * late))
            def _():
                pass_on(shared, way, 0)

            i = s - SPREAD_SKEW * late

            @pl.when((late >= 0) & (i >= 0) & (i < pieces))
            def _():
                pass_on(routed, way, i)
        if s == lag:
            def _start():
                extra[2].wait()
                shared_gather()
            ready.append(_start)
            ready += [functools.partial(shared_down, c) for c in range(chunks)]
        if s >= lag and (s - lag + 1) % each == 0:
            l = (s - lag + 1) // each - 1

            def _begin(l=l):
                lowers[l].wait()
                gather(l)
            ready.append(_begin)
            for c in range(chunks):
                ready.append(functools.partial(routed_down, l, c))
                if l == local - 1 and c + 1 in cuts:
                    ready.append(functools.partial(swap_out, cuts.index(c + 1) - 1))
        quota = 3 if s < pieces + lag - 1 else len(ready)
        for task in ready[:quota]:
            task()
        ready = ready[quota:]

    for stage_of in (add_up, send_home, arrive):
        for q in (0, 1):
            stage_of(q)

    def finish(group, way, i):
        @pl.when(place[way] < n - 1)
        def _():
            partial_send(group, way, i).wait_send()

        @pl.when(place[way] > 0)
        def _():
            hidden_send(group, way, i).wait_send()

    def drain(i, carry):
        for way in (0, 1):
            finish(routed, way, i)
        return carry

    lax.fori_loop(0, pieces, drain, 0)
    for way in (0, 1):
        finish(shared, way, 0)
    for copy in sends:
        copy.wait_send()


def layer(tokens, ids, weights, gate, up, down, sgate, sup, sdown, n, g):
    rows, model = tokens.shape
    width = model // n
    local, _, hidden = gate.shape
    experts = local * g
    thin = hidden // g
    wire = BF16 if n <= 4 else F32
    sliced = thin % 128 != 0
    if sliced:
        e = lax.axis_index("expert")
        sgate = lax.dynamic_slice_in_dim(sgate, e * thin, thin, 1)
        sup = lax.dynamic_slice_in_dim(sup, e * thin, thin, 1)
        sdown = lax.dynamic_slice_in_dim(sdown, e * thin, thin, 0)
    count = n * g * PITCH
    tiles = count // TILE
    slots = TILE // PITCH * CAP
    blocks = local * (hidden // COLS // 2)
    pieces = blocks * tiles * (slots // ROWS)
    half = n * g * rows // 2
    pool = n // 2
    ring = min(AHEAD + 1, blocks)
    return pl.pallas_call(
        functools.partial(layer_kernel, n, g, sliced),
        out_shape=jax.ShapeDtypeStruct((rows, model), BF16),
        in_specs=[VMEM] * 3 + [HBM] * 6,
        out_specs=VMEM,
        scratch_shapes=[
            pltpu.VMEM((n, g, rows, width), BF16),
            pltpu.VMEM((n, g, rows, experts), F32),
            pltpu.VMEM((rows, experts), F32),
            pltpu.VMEM((count, width), BF16),
            pltpu.VMEM((count, experts), F32),
            pltpu.VMEM((ring, width, 2 * COLS), BF16),
            pltpu.VMEM((ring, width, 2 * COLS), BF16),
            pltpu.VMEM((local, hidden, width), BF16),
            pltpu.VMEM((width, thin), BF16),
            pltpu.VMEM((width, thin), BF16),
            pltpu.VMEM((thin, width), BF16),
            pltpu.VMEM((tiles, slots, width), BF16),
            pltpu.VMEM((TILE // PITCH * rows, width), BF16),
            pltpu.VMEM((count, hidden), BF16),
            pltpu.VMEM((count, thin), BF16),
            pltpu.VMEM((n, g, PITCH, width), F32),
            pltpu.VMEM((local, count, 1), F32),
            pltpu.VMEM((2, pieces, 2, ROWS, COLS), F32),
            pltpu.VMEM((2, pieces, 2, ROWS, COLS), wire),
            pltpu.VMEM((2, pieces, 2, ROWS, COLS) if wire == BF16 else (8, 128), wire),
            pltpu.VMEM((2, pieces, ROWS, COLS), BF16),
            pltpu.VMEM((2, 1, 2, half, thin), F32),
            pltpu.VMEM((2, 1, 2, half, thin), wire),
            pltpu.VMEM((2, 1, 2, half, thin), wire),
            pltpu.VMEM((2, 1, half, thin), BF16),
            pltpu.VMEM((tiles, local, slots, TILE), BF16),
            pltpu.VMEM((tiles, local, TILE, slots), BF16),
            pltpu.VMEM((g, pool, PITCH, width), F32),
            pltpu.VMEM((pool, rows, width), F32),
            pltpu.VMEM((g, pool, rows, width), BF16),
            pltpu.VMEM((g, pool, rows, width), BF16),
            pltpu.VMEM((pool, rows, width), BF16),
            DMA((2, blocks)), DMA((local,)), DMA((3,)),
            DMA((2, pieces)), DMA((2, pieces)), DMA((2, pieces)), DMA((2, pieces)),
            DMA((2, 1)), DMA((2, 1)), DMA((2, 1)), DMA((2, 1)),
            DMA((2,)), DMA((2, n)), DMA((2, n)), DMA((2, n, g)), DMA((2, n, g)), DMA((n, g)), DMA((n, g)),
            DMA((2, g)), DMA((2, g)), DMA((2, g)), DMA((2, g)), DMA((2, pool, 2)), DMA((2, n)), DMA((2,)),
        ],
        compiler_params=pltpu.CompilerParams(
            collective_id=0, has_side_effects=True, vmem_limit_bytes=67043328
        ),
    )(tokens, ids, weights, gate, up, down, sgate, sup, sdown)


def per_device(
    tokens, expert_ids, route_weights, gate_weights, up_weights, down_weights,
    shared_gate, shared_up, shared_down,
):
    g, n = lax.axis_size("expert"), lax.axis_size("dp")
    return layer(
        tokens, expert_ids.T, route_weights.T, gate_weights, up_weights, down_weights,
        shared_gate, shared_up, shared_down, n, g,
    )


def solution(mesh):
    placed = (
        P(("dp", "expert"), None),
        P(("dp", "expert"), None),
        P(("dp", "expert"), None),
        P("expert", "dp", "tensor"),
        P("expert", "dp", "tensor"),
        P("expert", "tensor", "dp"),
        P("dp", "tensor"),
        P("dp", "tensor"),
        P("tensor", "dp"),
    )
    return jax.shard_map(
        per_device, mesh=mesh, in_specs=placed, out_specs=P(("dp", "expert"), None), check_vma=False
    )
```

```python
import functools

import jax
import jax.numpy as jnp
from jax import lax
from jax.experimental import pallas as pl
from jax.experimental.pallas import tpu as pltpu
from jax.sharding import PartitionSpec as P

CAP = 8
PITCH = 16
TILE = 256
COLS = 256
ROWS = 64
AHEAD = 3
SKEW = 5
SPREAD_SKEW = 5
MESH = pl.DeviceIdType.MESH
VMEM = pl.BlockSpec(memory_space=pltpu.VMEM)
HBM = pl.BlockSpec(memory_space=pl.ANY)
DMA = pltpu.SemaphoreType.DMA
F32 = jnp.float32
BF16 = jnp.bfloat16


def greet(peers):
    barrier = pltpu.get_barrier_semaphore()
    for peer in peers:
        pl.semaphore_signal(barrier, inc=1, device_id=peer, device_id_type=MESH)
    pl.semaphore_wait(barrier, len(peers))


def remote(src, dst, send, recv, peer):
    return pltpu.make_async_remote_copy(
        src_ref=src, dst_ref=dst, send_sem=send, recv_sem=recv, device_id=peer, device_id_type=MESH
    )


def packed(v, wire):
    return v if wire == F32 else (v * jnp.abs(v)).astype(wire)


def unpacked(v):
    if v.dtype == F32:
        return v
    v = v.astype(F32)
    size = jnp.abs(v)
    root = size * lax.rsqrt(jnp.maximum(size, 1e-30))
    return jnp.where(v < 0.0, -root, root)


def dot(a, b):
    return jnp.dot(a, b, preferred_element_type=F32)


def layer_kernel(
    n, g, sliced, tok, ids, weights, gate, up, down, sgate, sup, sdown, o,
    x, w, coef, xs, ws, gbuf, ubuf, dbuf, sgbuf, subuf, sdbuf, picked, compact, spread, sspread, acc, factor,
    own, got, out, hid, sown, sgot, sout, shid, here, there, peer_in, kept, ship, plane, done,
    wsem, dsem, ssem, s1, r1, s2, r2, t1, q1, t2, q2,
    lsem, u1, v1, u2, v2, u3, v3, sa, ra, sb, rb, sc, rc, osem,
):
    d, e, t = lax.axis_index("dp"), lax.axis_index("expert"), lax.axis_index("tensor")
    other = 1 - t
    rows, width = x.shape[2:]
    experts = w.shape[3]
    local, hidden = gate.shape[0], gate.shape[2]
    thin = sgbuf.shape[1]
    wire = out.dtype
    tiles = xs.shape[0] // TILE
    slots = TILE // PITCH * CAP
    solid = TILE // PITCH * rows
    pairs = hidden // COLS // 2
    pieces = own.shape[1]
    blocks = local * pairs
    per = pieces // blocks
    place = (d, n - 1 - d)
    ahead = (jnp.minimum(d + 1, n - 1), jnp.maximum(d - 1, 0))
    behind = (jnp.maximum(d - 1, 0), jnp.minimum(d + 1, n - 1))

    def load(b):
        at, slot = b // pairs, lax.rem(b, gbuf.shape[0])
        wide = pl.ds(pl.multiple_of(lax.rem(b, pairs) * 2 * COLS, 2 * COLS), 2 * COLS)
        return [
            pltpu.make_async_copy(src.at[at, :, wide], dst.at[slot], wsem.at[h, b])
            for h, (src, dst) in enumerate(((gate, gbuf), (up, ubuf)))
        ]

    start = 0 if sliced else e * thin
    across = pl.ds(0, thin) if sliced else pl.ds(pl.multiple_of(start, thin), thin)
    extra = [
        pltpu.make_async_copy(sgate.at[:, across], sgbuf, ssem.at[0]),
        pltpu.make_async_copy(sup.at[:, across], subuf, ssem.at[1]),
        pltpu.make_async_copy(sdown.at[across, :], sdbuf, ssem.at[2]),
    ]
    lowers = [pltpu.make_async_copy(down.at[l], dbuf.at[l], dsem.at[l]) for l in range(local)]

    for copy in extra[:2]:
        copy.start()
    for b in range(min(AHEAD, blocks)):
        for copy in load(b):
            copy.start()

    split = (width // 2) % 128 == 0
    part_lanes = width // 2 if split else width
    lanes = pl.ds(pl.multiple_of(t * part_lanes, 128), part_lanes) if split else pl.ds(0, width)

    def columns(block, part):
        first = block * width + (t * part_lanes if part and split else 0)
        return tok.at[:, pl.ds(pl.multiple_of(first, 128), part_lanes if part else width)]

    mine = pltpu.make_async_copy(columns(d, False), x.at[d, e], lsem.at[0])
    mine.start()
    name = lax.broadcasted_iota(jnp.int32, coef.shape, 1)
    named, held = ids[...].T, weights[...].T
    total = jnp.zeros(coef.shape, F32)
    for k in range(ids.shape[0]):
        total = total + jnp.where(named[:, k:k + 1] == name, held[:, k:k + 1], 0.0)
    coef[...] = total
    greet(
        [{"tensor": other}]
        + [{"expert": lax.rem(e + j, g)} for j in range(1, g)]
        + [{"dp": lax.rem(d + k, n), "tensor": c} for k in range(1, n) for c in (0, 1)]
    )
    put = pltpu.make_async_copy(coef, w.at[d, e], lsem.at[1])
    put.start()
    sends = []
    for k in range(1, n):
        to = lax.rem(d + k, n)
        for src, dst, a in ((coef, w.at[d, e], 1), (columns(to, True), x.at[d, e, :, lanes], 0)):
            copy = remote(src, dst, u1.at[a, k], v1.at[a, k], {"dp": to})
            copy.start()
            sends.append(copy)

    def view(a, block, peer):
        return x.at[block, peer, :, lanes] if a == 0 else w.at[block, peer]

    def cross(k, j, block, peer):
        at = x.at[block, peer, :, lanes]
        return remote(at, at, u3.at[k, j], v3.at[k, j], {"tensor": other})

    xs[...] = jnp.zeros_like(xs)
    ws[...] = jnp.zeros_like(ws)
    for k in range(n):
        block = lax.rem(d - k + n, n)
        for a in (1, 0):
            if k == 0:
                (mine, put)[a].wait()
            else:
                at = view(a, block, e)
                remote(at, at, u1.at[a, k], v1.at[a, k], {"dp": d}).wait_recv()
            for j in range(1, g):
                at = view(a, block, e)
                copy = remote(at, at, u2.at[a, k, j], v2.at[a, k, j], {"expert": lax.rem(e + j, g)})
                copy.start()
                sends.append(copy)
        if split and k:
            copy = cross(k, 0, block, e)
            copy.start()
            sends.append(copy)

    def crossed(k, j, a):
        at = view(a, lax.rem(d - k + n, n), lax.rem(e - j + g, g))
        remote(at, at, u2.at[a, k, j], v2.at[a, k, j], {"expert": e}).wait_recv()

    for k in range(n):
        for j in range(1, g):
            crossed(k, j, 1)
    for i in range(n):
        for j in range(g):
            at = (i * g + j) * PITCH
            ws[at:at + rows, :] = w[i, j]

    def iota(shape, axis):
        return lax.broadcasted_iota(jnp.int32, shape, axis)

    token_row, token_col = iota((TILE, TILE), 0), iota((TILE, TILE), 1)
    same = token_row // PITCH == token_col // PITCH
    before = jnp.where(same & (token_row < token_col), 1.0, 0.0).astype(BF16)
    behind_in = jnp.where(same & (token_col < token_row), 1.0, 0.0).astype(BF16)
    spots = 16
    pick_rows = jnp.where(
        iota((spots, experts), 1) == e * local + iota((spots, experts), 0), 1.0, 0.0
    ).astype(BF16)
    base_row = iota((spots, TILE), 1) // PITCH * CAP
    base_col = iota((TILE, experts), 0) // PITCH * CAP
    for a in range(tiles):
        part = ws[a * TILE:(a + 1) * TILE, :]
        chosen = jnp.where(part > 0.0, 1.0, 0.0).astype(BF16)
        row = lax.dot_general(
            pick_rows, chosen, (((1,), (1,)), ((), ())), preferred_element_type=F32
        )
        rank_row = dot(row.astype(BF16), before).astype(jnp.int32)
        goal_row = jnp.where(row > 0.5, base_row + rank_row, -1)
        rank_col = dot(behind_in, chosen).astype(jnp.int32)
        goal_col = jnp.where(part > 0.0, base_col + rank_col, -1).astype(F32)
        for l in range(local):
            mark = iota((TILE, experts), 1) == e * local + l
            column = jnp.sum(jnp.where(mark, goal_col, 0.0), axis=1, keepdims=True)
            here[a, l] = jnp.where(
                goal_row[l:l + 1, :] == iota((slots, TILE), 0), 1.0, 0.0
            ).astype(BF16)
            there[a, l] = jnp.where(
                column.astype(jnp.int32) == iota((TILE, slots), 1), 1.0, 0.0
            ).astype(BF16)
            factor[l, a * TILE:(a + 1) * TILE, :] = jnp.sum(
                jnp.where(mark, part, 0.0), axis=1, keepdims=True
            )

    for k in range(n):
        for j in range(1, g):
            crossed(k, j, 0)
            if split:
                copy = cross(k, j, lax.rem(d - k + n, n), lax.rem(e - j + g, g))
                copy.start()
                sends.append(copy)
    if split:
        rest_lanes = pl.ds(pl.multiple_of(other * part_lanes, 128), part_lanes)
        for k in range(n):
            for j in range(g):
                if k or j:
                    at = x.at[lax.rem(d - k + n, n), lax.rem(e - j + g, g), :, rest_lanes]
                    remote(at, at, u3.at[k, j], v3.at[k, j], {"tensor": t}).wait_recv()
    for i in range(n):
        for j in range(g):
            at = (i * g + j) * PITCH
            xs[at:at + rows, :] = x[i, j]

    def solid_map(shape, slot_axis, token_axis):
        token, slot = iota(shape, token_axis), iota(shape, slot_axis)
        inside = token % PITCH
        return jnp.where(
            (inside < rows) & (token // PITCH * rows + inside == slot), 1.0, 0.0
        ).astype(BF16)

    rest = solid // 2
    pack_map = solid_map((solid, TILE), 0, 1)
    for a in range(tiles):
        compact[...] = dot(pack_map, xs[a * TILE:(a + 1) * TILE, :]).astype(BF16)
        if a == 0:
            for copy in extra[:2]:
                copy.wait()
        for h, buf in ((0, sgbuf), (1, subuf)):
            value = dot(compact[...], buf[...])
            for way in (0, 1):
                sown[way, 0, h, a * rest:(a + 1) * rest, :] = value[way * rest:(way + 1) * rest]

    routed = (own, got, out if wire == BF16 else own, hid, s1, r1, s2, r2)
    shared = (sown, sgot, sout if wire == BF16 else sown, shid, t1, q1, t2, q2)

    def partial_send(group, way, i):
        return remote(
            group[2].at[way, i], group[1].at[way, i], group[4].at[way, i], group[5].at[way, i],
            {"dp": ahead[way]},
        )

    def hidden_send(group, way, i):
        at = group[3].at[way, i]
        return remote(at, at, group[6].at[way, i], group[7].at[way, i], {"dp": behind[way]})

    def forward(group, way, i):
        mine, come, leave, final = group[:4]

        @pl.when(place[way] == 0)
        def _():
            if leave is not mine:
                for h in (0, 1):
                    leave[way, i, h] = packed(mine[way, i, h], wire)
            partial_send(group, way, i).start()

        @pl.when(place[way] > 0)
        def _():
            partial_send(group, way, i).wait_recv()

            @pl.when(place[way] < n - 1)
            def _():
                for h in (0, 1):
                    leave[way, i, h] = packed(mine[way, i, h] + unpacked(come[way, i, h]), wire)
                partial_send(group, way, i).start()

            @pl.when(place[way] == n - 1)
            def _():
                a, b = (mine[way, i, h] + unpacked(come[way, i, h]) for h in (0, 1))
                final[way, i] = (a / (1.0 + jnp.exp(-a)) * b).astype(final.dtype)
                hidden_send(group, way, i).start()

    def pass_on(group, way, i):
        hidden_send(group, way, i).wait_recv()

        @pl.when(place[way] > 0)
        def _():
            hidden_send(group, way, i).start()

    def project(b):
        at, slot = b // pairs, lax.rem(b, gbuf.shape[0])

        @pl.when(lax.rem(b, pairs) == 0)
        def _():
            for a in range(tiles):
                picked[a] = dot(here[a, at], xs[a * TILE:(a + 1) * TILE, :]).astype(BF16)

        for copy in load(b):
            copy.wait()

        @pl.when(b + AHEAD < blocks)
        def _():
            for copy in load(b + AHEAD):
                copy.start()

        @pl.when(b + AHEAD == blocks)
        def _():
            for copy in extra[2:] + lowers:
                copy.start()

        fine = slots // ROWS
        for h, buf in ((0, gbuf), (1, ubuf)):
            for a in range(tiles):
                value = dot(picked[a], buf[slot])
                for way in (0, 1):
                    for r in range(fine):
                        own[way, b * per + a * fine + r, h] = value[
                            r * ROWS:(r + 1) * ROWS, way * COLS:(way + 1) * COLS
                        ]

    def stage(s, carry):
        @pl.when(s < blocks)
        def _():
            project(s)

        for way in (0, 1):
            @pl.when(s == SKEW * place[way])
            def _():
                forward(shared, way, 0)

            i = s - SKEW * place[way]

            @pl.when((i >= 0) & (i < pieces))
            def _():
                forward(routed, way, i)
        return carry

    lax.fori_loop(0, pieces + SKEW * (n - 1), stage, 0)

    spans = [(lo, min(lo + 2 * TILE, width)) for lo in range(0, width, 2 * TILE)]
    chunks = len(spans)
    ready = []

    def gather(l):
        for way in (0, 1):
            for c in range(pairs):
                b = l * pairs + c
                fine = slots // ROWS
                for a in range(tiles):
                    value = hid[way, b * per + a * fine:b * per + (a + 1) * fine]
                    spread[a * TILE:(a + 1) * TILE, (2 * c + way) * COLS:(2 * c + way + 1) * COLS] = dot(
                        there[a, l], value.reshape(slots, COLS)
                    ).astype(BF16)

    def shared_gather():
        unpack_map = solid_map((TILE, solid), 1, 0)
        for a in range(tiles):
            value = jnp.concatenate([shid[way, 0, a * rest:(a + 1) * rest] for way in (0, 1)], axis=0)
            sspread[a * TILE:(a + 1) * TILE, :] = dot(unpack_map, value).astype(BF16)

    deep = TILE // PITCH // g

    def shared_down(c):
        at = slice(*spans[c])
        for a in range(tiles):
            span = slice(a * TILE, (a + 1) * TILE)
            value = dot(sspread[span, :], sdbuf[:, at])
            acc[a * deep:(a + 1) * deep, :, :, at] = value.reshape(deep, g, PITCH, -1)

    def routed_down(l, c):
        at = slice(*spans[c])
        for a in range(tiles):
            span = slice(a * TILE, (a + 1) * TILE)
            value = factor[l, span, :] * dot(spread[span, :], dbuf[l, :, at])
            acc[a * deep:(a + 1) * deep, :, :, at] += value.reshape(deep, g, PITCH, -1)

    pool = n // 2
    cuts = list(range(chunks + 1))
    groups = spans
    order = list(range(1, g)) + [0]

    def swap(q, j):
        lo, hi = groups[q]
        to = lax.rem(e + j, g)
        return remote(
            acc.at[pl.ds(other * pool, pool), to, :, pl.ds(lo, hi - lo)],
            peer_in.at[to, :, :, pl.ds(lo, hi - lo)], sa.at[q, j], ra.at[q, j], {"tensor": other},
        )

    def ship_to(q, j):
        lo, hi = groups[q]
        return remote(
            ship.at[j, :, :, pl.ds(lo, hi - lo)], plane.at[j, :, :, pl.ds(lo, hi - lo)],
            sb.at[q, j], rb.at[q, j], {"expert": lax.rem(e + j, g)},
        )

    def swap_out(q):
        for j in order:
            swap(q, j).start()

    def add_up(q):
        lo, hi = groups[q]
        for j in order:
            to = lax.rem(e + j, g)
            swap(q, j).wait_recv()
            value = acc[pl.ds(t * pool, pool), to, :, lo:hi] + peer_in[to, :, :, lo:hi]
            value = value[:, :rows]
            if j:
                ship[j, :, :, lo:hi] = packed(value, ship.dtype)
                ship_to(q, j).start()
            else:
                kept[:, :, lo:hi] = value

    def goal(q, block):
        lo, hi = groups[q]
        return o.at[:, pl.ds(pl.multiple_of(block * width + lo, 128), hi - lo)]

    def home_send(q, i):
        lo, hi = groups[q]
        home = t * pool + i
        src = done.at[i, :, pl.ds(lo, hi - lo)]
        copies = []
        for c in (0, 1):
            inside = (home == d) & (t == c)
            away = remote(src, goal(q, d), sc.at[q, i, c], rc.at[q, d], {"dp": home, "tensor": c})
            local_copy = pltpu.make_async_copy(src, goal(q, d), osem.at[q])
            copies.append((inside, away, local_copy))
        return copies

    def send_home(q):
        lo, hi = groups[q]
        value = kept[:, :, lo:hi]
        for j in range(1, g):
            ship_to(q, j).wait_recv()
            value = value + unpacked(plane[j, :, :, lo:hi])
        done[:, :, lo:hi] = value.astype(done.dtype)
        for i in range(pool):
            for inside, away, local_copy in home_send(q, i):
                pl.when(jnp.logical_not(inside))(away.start)
                pl.when(inside)(local_copy.start)

    def arrive(q):
        for k in range(n):
            stays = (d // pool == t) & (d == k)

            @pl.when(jnp.logical_not(stays))
            def _():
                lo, hi = groups[q]
                remote(
                    done.at[0, :, pl.ds(lo, hi - lo)], goal(q, k), sc.at[q, 0, 0], rc.at[q, k], {"dp": d}
                ).wait_recv()
        for i in range(pool):
            for inside, away, local_copy in home_send(q, i):
                pl.when(jnp.logical_not(inside))(away.wait_send)
                pl.when(inside)(local_copy.wait)
        for j in order:
            swap(q, j).wait_send()
            if j:
                ship_to(q, j).wait_send()

    lag = SPREAD_SKEW * (n - 2)
    each = pieces // local
    for s in range(pieces + lag):
        for way in (0, 1):
            late = n - 2 - place[way]

            @pl.when((late >= 0) & (s == SPREAD_SKEW * late))
            def _():
                pass_on(shared, way, 0)

            i = s - SPREAD_SKEW * late

            @pl.when((late >= 0) & (i >= 0) & (i < pieces))
            def _():
                pass_on(routed, way, i)
        if s == lag:
            def _start():
                extra[2].wait()
                shared_gather()
            ready.append(_start)
            ready += [functools.partial(shared_down, c) for c in range(chunks)]
        if s >= lag and (s - lag + 1) % each == 0:
            l = (s - lag + 1) // each - 1

            def _begin(l=l):
                lowers[l].wait()
                gather(l)
            ready.append(_begin)
            for c in range(chunks):
                ready.append(functools.partial(routed_down, l, c))
                if l == local - 1 and c + 1 in cuts:
                    ready.append(functools.partial(swap_out, cuts.index(c + 1) - 1))
        quota = 3 if s < pieces + lag - 1 else len(ready)
        for task in ready[:quota]:
            task()
        ready = ready[quota:]

    for stage_of in (add_up, send_home, arrive):
        for q in range(chunks):
            stage_of(q)

    def finish(group, way, i):
        @pl.when(place[way] < n - 1)
        def _():
            partial_send(group, way, i).wait_send()

        @pl.when(place[way] > 0)
        def _():
            hidden_send(group, way, i).wait_send()

    def drain(i, carry):
        for way in (0, 1):
            finish(routed, way, i)
        return carry

    lax.fori_loop(0, pieces, drain, 0)
    for way in (0, 1):
        finish(shared, way, 0)
    for copy in sends:
        copy.wait_send()


def layer(tokens, ids, weights, gate, up, down, sgate, sup, sdown, n, g):
    rows, model = tokens.shape
    width = model // n
    local, _, hidden = gate.shape
    experts = local * g
    thin = hidden // g
    wire = BF16 if n <= 4 else F32
    sliced = thin % 128 != 0
    if sliced:
        e = lax.axis_index("expert")
        sgate = lax.dynamic_slice_in_dim(sgate, e * thin, thin, 1)
        sup = lax.dynamic_slice_in_dim(sup, e * thin, thin, 1)
        sdown = lax.dynamic_slice_in_dim(sdown, e * thin, thin, 0)
    count = n * g * PITCH
    tiles = count // TILE
    slots = TILE // PITCH * CAP
    blocks = local * (hidden // COLS // 2)
    pieces = blocks * tiles * (slots // ROWS)
    half = n * g * rows // 2
    pool = n // 2
    ring = min(AHEAD + 1, blocks)
    parts = -(-width // (2 * TILE))
    return pl.pallas_call(
        functools.partial(layer_kernel, n, g, sliced),
        out_shape=jax.ShapeDtypeStruct((rows, model), BF16),
        in_specs=[VMEM] * 3 + [HBM] * 6,
        out_specs=VMEM,
        scratch_shapes=[
            pltpu.VMEM((n, g, rows, width), BF16),
            pltpu.VMEM((n, g, rows, experts), F32),
            pltpu.VMEM((rows, experts), F32),
            pltpu.VMEM((count, width), BF16),
            pltpu.VMEM((count, experts), F32),
            pltpu.VMEM((ring, width, 2 * COLS), BF16),
            pltpu.VMEM((ring, width, 2 * COLS), BF16),
            pltpu.VMEM((local, hidden, width), BF16),
            pltpu.VMEM((width, thin), BF16),
            pltpu.VMEM((width, thin), BF16),
            pltpu.VMEM((thin, width), BF16),
            pltpu.VMEM((tiles, slots, width), BF16),
            pltpu.VMEM((TILE // PITCH * rows, width), BF16),
            pltpu.VMEM((count, hidden), BF16),
            pltpu.VMEM((count, thin), BF16),
            pltpu.VMEM((n, g, PITCH, width), F32),
            pltpu.VMEM((local, count, 1), F32),
            pltpu.VMEM((2, pieces, 2, ROWS, COLS), F32),
            pltpu.VMEM((2, pieces, 2, ROWS, COLS), wire),
            pltpu.VMEM((2, pieces, 2, ROWS, COLS) if wire == BF16 else (8, 128), wire),
            pltpu.VMEM((2, pieces, ROWS, COLS), BF16),
            pltpu.VMEM((2, 1, 2, half, thin), F32),
            pltpu.VMEM((2, 1, 2, half, thin), wire),
            pltpu.VMEM((2, 1, 2, half, thin), wire),
            pltpu.VMEM((2, 1, half, thin), BF16),
            pltpu.VMEM((tiles, local, slots, TILE), BF16),
            pltpu.VMEM((tiles, local, TILE, slots), BF16),
            pltpu.VMEM((g, pool, PITCH, width), F32),
            pltpu.VMEM((pool, rows, width), F32),
            pltpu.VMEM((g, pool, rows, width), BF16),
            pltpu.VMEM((g, pool, rows, width), BF16),
            pltpu.VMEM((pool, rows, width), BF16),
            DMA((2, blocks)), DMA((local,)), DMA((3,)),
            DMA((2, pieces)), DMA((2, pieces)), DMA((2, pieces)), DMA((2, pieces)),
            DMA((2, 1)), DMA((2, 1)), DMA((2, 1)), DMA((2, 1)),
            DMA((2,)), DMA((2, n)), DMA((2, n)), DMA((2, n, g)), DMA((2, n, g)), DMA((n, g)), DMA((n, g)),
            DMA((parts, g)), DMA((parts, g)), DMA((parts, g)), DMA((parts, g)),
            DMA((parts, pool, 2)), DMA((parts, n)), DMA((parts,)),
        ],
        compiler_params=pltpu.CompilerParams(
            collective_id=0, has_side_effects=True, vmem_limit_bytes=67043328
        ),
    )(tokens, ids, weights, gate, up, down, sgate, sup, sdown)


def per_device(
    tokens, expert_ids, route_weights, gate_weights, up_weights, down_weights,
    shared_gate, shared_up, shared_down,
):
    g, n = lax.axis_size("expert"), lax.axis_size("dp")
    return layer(
        tokens, expert_ids.T, route_weights.T, gate_weights, up_weights, down_weights,
        shared_gate, shared_up, shared_down, n, g,
    )


def solution(mesh):
    placed = (
        P(("dp", "expert"), None),
        P(("dp", "expert"), None),
        P(("dp", "expert"), None),
        P("expert", "dp", "tensor"),
        P("expert", "dp", "tensor"),
        P("expert", "tensor", "dp"),
        P("dp", "tensor"),
        P("dp", "tensor"),
        P("tensor", "dp"),
    )
    return jax.shard_map(
        per_device, mesh=mesh, in_specs=placed, out_specs=P(("dp", "expert"), None), check_vma=False
    )
```

```python
import functools

import jax
import jax.numpy as jnp
from jax import lax
from jax.experimental import pallas as pl
from jax.experimental.pallas import tpu as pltpu
from jax.sharding import PartitionSpec as P

CAP = 8
PITCH = 16
TILE = 256
COLS = 256
ROWS = 64
AHEAD = 3
SKEW = 4
SPREAD_SKEW = 5
MESH = pl.DeviceIdType.MESH
VMEM = pl.BlockSpec(memory_space=pltpu.VMEM)
HBM = pl.BlockSpec(memory_space=pl.ANY)
DMA = pltpu.SemaphoreType.DMA
F32 = jnp.float32
BF16 = jnp.bfloat16


def greet(peers):
    barrier = pltpu.get_barrier_semaphore()
    for peer in peers:
        pl.semaphore_signal(barrier, inc=1, device_id=peer, device_id_type=MESH)
    pl.semaphore_wait(barrier, len(peers))


def remote(src, dst, send, recv, peer):
    return pltpu.make_async_remote_copy(
        src_ref=src, dst_ref=dst, send_sem=send, recv_sem=recv, device_id=peer, device_id_type=MESH
    )


def packed(v, wire):
    return v if wire == F32 else (v * jnp.abs(v)).astype(wire)


def unpacked(v):
    if v.dtype == F32:
        return v
    v = v.astype(F32)
    size = jnp.abs(v)
    root = size * lax.rsqrt(jnp.maximum(size, 1e-30))
    return jnp.where(v < 0.0, -root, root)


def dot(a, b):
    return jnp.dot(a, b, preferred_element_type=F32)


def layer_kernel(
    n, g, sliced, tok, ids, weights, gate, up, down, sgate, sup, sdown, o,
    x, w, coef, xs, ws, gbuf, ubuf, dbuf, sgbuf, subuf, sdbuf, picked, compact, spread, sspread, acc, factor,
    own, got, out, hid, sown, sgot, sout, shid, here, there, peer_in, kept, ship, plane, done,
    wsem, dsem, ssem, s1, r1, s2, r2, t1, q1, t2, q2,
    lsem, u1, v1, u2, v2, u3, v3, sa, ra, sb, rb, sc, rc, osem,
):
    d, e, t = lax.axis_index("dp"), lax.axis_index("expert"), lax.axis_index("tensor")
    other = 1 - t
    rows, width = x.shape[2:]
    experts = w.shape[3]
    local, hidden = gate.shape[0], gate.shape[2]
    thin = sgbuf.shape[1]
    wire = out.dtype
    tiles = xs.shape[0] // TILE
    pool, few = n // 2, n // 4
    at_home = list(range(few)) + list(range(n - few, n)) + list(range(few, n - few))
    position = [at_home.index(i) for i in range(n)]
    slots = TILE // PITCH * CAP
    solid = TILE // PITCH * rows
    pairs = hidden // COLS // 2
    pieces = own.shape[1]
    blocks = local * pairs
    per = pieces // blocks
    place = (d, n - 1 - d)
    ahead = (jnp.minimum(d + 1, n - 1), jnp.maximum(d - 1, 0))
    behind = (jnp.maximum(d - 1, 0), jnp.minimum(d + 1, n - 1))

    def load(b):
        at, slot = b // pairs, lax.rem(b, gbuf.shape[0])
        wide = pl.ds(pl.multiple_of(lax.rem(b, pairs) * 2 * COLS, 2 * COLS), 2 * COLS)
        return [
            pltpu.make_async_copy(src.at[at, :, wide], dst.at[slot], wsem.at[h, b])
            for h, (src, dst) in enumerate(((gate, gbuf), (up, ubuf)))
        ]

    start = 0 if sliced else e * thin
    across = pl.ds(0, thin) if sliced else pl.ds(pl.multiple_of(start, thin), thin)
    extra = [
        pltpu.make_async_copy(sgate.at[:, across], sgbuf, ssem.at[0]),
        pltpu.make_async_copy(sup.at[:, across], subuf, ssem.at[1]),
        pltpu.make_async_copy(sdown.at[across, :], sdbuf, ssem.at[2]),
    ]
    lowers = [pltpu.make_async_copy(down.at[l], dbuf.at[l], dsem.at[l]) for l in range(local)]

    for copy in extra[:2]:
        copy.start()
    for b in range(min(AHEAD, blocks)):
        for copy in load(b):
            copy.start()

    split = (width // 2) % 128 == 0
    part_lanes = width // 2 if split else width
    lanes = pl.ds(pl.multiple_of(t * part_lanes, 128), part_lanes) if split else pl.ds(0, width)

    def columns(block, part):
        first = block * width + (t * part_lanes if part and split else 0)
        return tok.at[:, pl.ds(pl.multiple_of(first, 128), part_lanes if part else width)]

    mine = pltpu.make_async_copy(columns(d, False), x.at[d, e], lsem.at[0])
    mine.start()
    name = lax.broadcasted_iota(jnp.int32, coef.shape, 1)
    named, held = ids[...].T, weights[...].T
    total = jnp.zeros(coef.shape, F32)
    for k in range(ids.shape[0]):
        total = total + jnp.where(named[:, k:k + 1] == name, held[:, k:k + 1], 0.0)
    coef[...] = total
    greet(
        [{"tensor": other}]
        + [{"expert": lax.rem(e + j, g)} for j in range(1, g)]
        + [{"dp": lax.rem(d + k, n), "tensor": c} for k in range(1, n) for c in (0, 1)]
    )
    put = pltpu.make_async_copy(coef, w.at[d, e], lsem.at[1])
    put.start()
    sends = []
    for k in range(1, n):
        to = lax.rem(d + k, n)
        for src, dst, a in ((coef, w.at[d, e], 1), (columns(to, True), x.at[d, e, :, lanes], 0)):
            copy = remote(src, dst, u1.at[a, k], v1.at[a, k], {"dp": to})
            copy.start()
            sends.append(copy)

    def view(a, block, peer):
        return x.at[block, peer, :, lanes] if a == 0 else w.at[block, peer]

    def cross(k, j, block, peer):
        at = x.at[block, peer, :, lanes]
        return remote(at, at, u3.at[k, j], v3.at[k, j], {"tensor": other})

    xs[...] = jnp.zeros_like(xs)
    ws[...] = jnp.zeros_like(ws)
    for k in range(n):
        block = lax.rem(d - k + n, n)
        for a in (1, 0):
            if k == 0:
                (mine, put)[a].wait()
            else:
                at = view(a, block, e)
                remote(at, at, u1.at[a, k], v1.at[a, k], {"dp": d}).wait_recv()
            for j in range(1, g):
                at = view(a, block, e)
                copy = remote(at, at, u2.at[a, k, j], v2.at[a, k, j], {"expert": lax.rem(e + j, g)})
                copy.start()
                sends.append(copy)
        if split and k:
            copy = cross(k, 0, block, e)
            copy.start()
            sends.append(copy)

    def crossed(k, j, a):
        at = view(a, lax.rem(d - k + n, n), lax.rem(e - j + g, g))
        remote(at, at, u2.at[a, k, j], v2.at[a, k, j], {"expert": e}).wait_recv()

    for k in range(n):
        for j in range(1, g):
            crossed(k, j, 1)
    for i in range(n):
        for j in range(g):
            at = (position[i] * g + j) * PITCH
            ws[at:at + rows, :] = w[i, j]

    def iota(shape, axis):
        return lax.broadcasted_iota(jnp.int32, shape, axis)

    token_row, token_col = iota((TILE, TILE), 0), iota((TILE, TILE), 1)
    same = token_row // PITCH == token_col // PITCH
    before = jnp.where(same & (token_row < token_col), 1.0, 0.0).astype(BF16)
    behind_in = jnp.where(same & (token_col < token_row), 1.0, 0.0).astype(BF16)
    spots = 16
    pick_rows = jnp.where(
        iota((spots, experts), 1) == e * local + iota((spots, experts), 0), 1.0, 0.0
    ).astype(BF16)
    base_row = iota((spots, TILE), 1) // PITCH * CAP
    base_col = iota((TILE, experts), 0) // PITCH * CAP
    for a in range(tiles):
        part = ws[a * TILE:(a + 1) * TILE, :]
        chosen = jnp.where(part > 0.0, 1.0, 0.0).astype(BF16)
        row = lax.dot_general(
            pick_rows, chosen, (((1,), (1,)), ((), ())), preferred_element_type=F32
        )
        rank_row = dot(row.astype(BF16), before).astype(jnp.int32)
        goal_row = jnp.where(row > 0.5, base_row + rank_row, -1)
        rank_col = dot(behind_in, chosen).astype(jnp.int32)
        goal_col = jnp.where(part > 0.0, base_col + rank_col, -1).astype(F32)
        for l in range(local):
            mark = iota((TILE, experts), 1) == e * local + l
            column = jnp.sum(jnp.where(mark, goal_col, 0.0), axis=1, keepdims=True)
            here[a, l] = jnp.where(
                goal_row[l:l + 1, :] == iota((slots, TILE), 0), 1.0, 0.0
            ).astype(BF16)
            for r in range(slots // ROWS):
                piece = column[r * 2 * ROWS:(r + 1) * 2 * ROWS].astype(jnp.int32) - r * ROWS
                there[a * (slots // ROWS) + r, l] = jnp.where(
                    piece == iota((2 * ROWS, ROWS), 1), 1.0, 0.0
                ).astype(BF16)
            factor[l, a * TILE:(a + 1) * TILE, :] = jnp.sum(
                jnp.where(mark, part, 0.0), axis=1, keepdims=True
            )

    for k in range(n):
        for j in range(1, g):
            crossed(k, j, 0)
            if split:
                copy = cross(k, j, lax.rem(d - k + n, n), lax.rem(e - j + g, g))
                copy.start()
                sends.append(copy)
    if split:
        rest_lanes = pl.ds(pl.multiple_of(other * part_lanes, 128), part_lanes)
        for k in range(n):
            for j in range(g):
                if k or j:
                    at = x.at[lax.rem(d - k + n, n), lax.rem(e - j + g, g), :, rest_lanes]
                    remote(at, at, u3.at[k, j], v3.at[k, j], {"tensor": t}).wait_recv()
    for i in range(n):
        for j in range(g):
            at = (position[i] * g + j) * PITCH
            xs[at:at + rows, :] = x[i, j]

    def solid_map(shape, slot_axis, token_axis):
        token, slot = iota(shape, token_axis), iota(shape, slot_axis)
        inside = token % PITCH
        return jnp.where(
            (inside < rows) & (token // PITCH * rows + inside == slot), 1.0, 0.0
        ).astype(BF16)

    rest = solid // 2
    pack_map = solid_map((solid, TILE), 0, 1)
    for a in range(tiles):
        compact[...] = dot(pack_map, xs[a * TILE:(a + 1) * TILE, :]).astype(BF16)
        if a == 0:
            for copy in extra[:2]:
                copy.wait()
        for h, buf in ((0, sgbuf), (1, subuf)):
            value = dot(compact[...], buf[...])
            for way in (0, 1):
                sown[way, 0, h, a * rest:(a + 1) * rest, :] = value[way * rest:(way + 1) * rest]

    routed = (own, got, out if wire == BF16 else own, hid, s1, r1, s2, r2)
    shared = (sown, sgot, sout if wire == BF16 else sown, shid, t1, q1, t2, q2)

    def partial_send(group, way, i):
        return remote(
            group[2].at[way, i], group[1].at[way, i], group[4].at[way, i], group[5].at[way, i],
            {"dp": ahead[way]},
        )

    def hidden_send(group, way, i):
        at = group[3].at[way, i]
        return remote(at, at, group[6].at[way, i], group[7].at[way, i], {"dp": behind[way]})

    def forward(group, way, i):
        mine, come, leave, final = group[:4]

        @pl.when(place[way] == 0)
        def _():
            if leave is not mine:
                for h in (0, 1):
                    leave[way, i, h] = packed(mine[way, i, h], wire)
            partial_send(group, way, i).start()

        @pl.when(place[way] > 0)
        def _():
            partial_send(group, way, i).wait_recv()

            @pl.when(place[way] < n - 1)
            def _():
                for h in (0, 1):
                    leave[way, i, h] = packed(mine[way, i, h] + unpacked(come[way, i, h]), wire)
                partial_send(group, way, i).start()

            @pl.when(place[way] == n - 1)
            def _():
                a, b = (mine[way, i, h] + unpacked(come[way, i, h]) for h in (0, 1))
                final[way, i] = (a / (1.0 + jnp.exp(-a)) * b).astype(final.dtype)
                hidden_send(group, way, i).start()

    def pass_on(group, way, i):
        hidden_send(group, way, i).wait_recv()

        @pl.when(place[way] > 0)
        def _():
            hidden_send(group, way, i).start()

    def project(b):
        at, slot = b // pairs, lax.rem(b, gbuf.shape[0])

        @pl.when(lax.rem(b, pairs) == 0)
        def _():
            for a in range(tiles):
                picked[a] = dot(here[a, at], xs[a * TILE:(a + 1) * TILE, :]).astype(BF16)

        for copy in load(b):
            copy.wait()

        @pl.when(b + AHEAD < blocks)
        def _():
            for copy in load(b + AHEAD):
                copy.start()

        @pl.when(b + AHEAD == blocks)
        def _():
            for copy in extra[2:] + lowers:
                copy.start()

        fine = slots // ROWS
        for h, buf in ((0, gbuf), (1, ubuf)):
            for a in range(tiles):
                value = dot(picked[a], buf[slot])
                for way in (0, 1):
                    for r in range(fine):
                        own[way, (a * fine + r) * blocks + b, h] = value[
                            r * ROWS:(r + 1) * ROWS, way * COLS:(way + 1) * COLS
                        ]

    def stage(s, carry):
        @pl.when(s < blocks)
        def _():
            project(s)

        for way in (0, 1):
            @pl.when(s == SKEW * place[way])
            def _():
                forward(shared, way, 0)

            i = s - SKEW * place[way]

            @pl.when((i >= 0) & (i < pieces))
            def _():
                forward(routed, way, i)
        return carry

    lax.fori_loop(0, pieces + SKEW * (n - 1), stage, 0)

    spans = [(lo, min(lo + 2 * TILE, width)) for lo in range(0, width, 2 * TILE)]
    chunks = len(spans)
    ready = []

    tall = 2 * ROWS
    stack = tall // PITCH

    def gather(r, l):
        for u in range(r * per // 2, (r + 1) * per // 2):
            for way in (0, 1):
                for c in range(pairs):
                    spread[u * tall:(u + 1) * tall, (2 * c + way) * COLS:(2 * c + way + 1) * COLS] = dot(
                        there[u, l], hid[way, u * blocks + l * pairs + c]
                    ).astype(BF16)

    def shared_gather():
        unpack_map = solid_map((TILE, solid), 1, 0)
        for a in range(tiles):
            value = jnp.concatenate([shid[way, 0, a * rest:(a + 1) * rest] for way in (0, 1)], axis=0)
            sspread[a * TILE:(a + 1) * TILE, :] = dot(unpack_map, value).astype(BF16)

    def shared_down(c):
        at = slice(*spans[c])
        for u in range(per):
            value = dot(sspread[u * tall:(u + 1) * tall, :], sdbuf[:, at])
            acc[u * stack:(u + 1) * stack, :, at] = value.reshape(stack, PITCH, -1)

    def routed_down(r, l, c):
        at = slice(*spans[c])
        for u in range(r * per // 2, (r + 1) * per // 2):
            span = slice(u * tall, (u + 1) * tall)
            value = factor[l, span, :] * dot(spread[span, :], dbuf[l, :, at])
            acc[u * stack:(u + 1) * stack, :, at] += value.reshape(stack, PITCH, -1)

    middle = spans[(chunks - 1) // 2][1]
    groups = [(0, 0, width), (1, 0, middle), (1, middle, width)]
    order = list(range(1, g)) + [0]

    def spot(r, core, i):
        return r * pool + core * few + i

    def home_of(r, core, i):
        return few + core * few + i if r else core * (n - few) + i

    def swap(q, j, i):
        r, lo, hi = groups[q]
        to = lax.rem(e + j, g)
        cols = pl.ds(lo, hi - lo)
        return remote(
            acc.at[spot(r, other, i) * g + to, :, cols], peer_in.at[r, to, i, :, cols],
            sa.at[q, j, i], ra.at[q, j, i], {"tensor": other},
        )

    def ship_to(q, j):
        r, lo, hi = groups[q]
        cols = pl.ds(lo, hi - lo)
        return remote(
            ship.at[r, j, :, :, cols], plane.at[r, j, :, :, cols],
            sb.at[q, j], rb.at[q, j], {"expert": lax.rem(e + j, g)},
        )

    def swap_out(q):
        for j in order:
            for i in range(few):
                swap(q, j, i).start()

    def add_up(q):
        r, lo, hi = groups[q]
        for j in order:
            to = lax.rem(e + j, g)
            for i in range(few):
                swap(q, j, i).wait_recv()
                value = acc[spot(r, t, i) * g + to, :, lo:hi] + peer_in[r, to, i, :, lo:hi]
                if j:
                    ship[r, j, i, :, lo:hi] = packed(value[:rows], ship.dtype)
                else:
                    kept[r, i, :, lo:hi] = value[:rows]
            if j:
                ship_to(q, j).start()

    def goal(q, block):
        r, lo, hi = groups[q]
        return o.at[:, pl.ds(pl.multiple_of(block * width + lo, 128), hi - lo)]

    def home_send(q, i):
        r, lo, hi = groups[q]
        home = home_of(r, t, i)
        src = done.at[r, i, :, pl.ds(lo, hi - lo)]
        copies = []
        for c in (0, 1):
            inside = (home == d) & (t == c)
            away = remote(src, goal(q, d), sc.at[q, i, c], rc.at[q, d], {"dp": home, "tensor": c})
            local_copy = pltpu.make_async_copy(src, goal(q, d), osem.at[q])
            copies.append((inside, away, local_copy))
        return copies

    def send_home(q):
        r, lo, hi = groups[q]
        for j in range(1, g):
            ship_to(q, j).wait_recv()
        for i in range(few):
            value = kept[r, i, :, lo:hi]
            for j in range(1, g):
                value = value + unpacked(plane[r, j, i, :, lo:hi])
            done[r, i, :, lo:hi] = value.astype(done.dtype)
            for inside, away, local_copy in home_send(q, i):
                pl.when(jnp.logical_not(inside))(away.start)
                pl.when(inside)(local_copy.start)

    inner = (d >= few) & (d < n - few)
    upper = jnp.where(d >= pool, 1, 0)

    def arrive(q):
        r, lo, hi = groups[q]
        now = inner if r else jnp.logical_not(inner)
        for k in range(n):
            stays = (upper == t) & (d == k)

            @pl.when(now & jnp.logical_not(stays))
            def _():
                remote(
                    done.at[r, 0, :, pl.ds(lo, hi - lo)], goal(q, k), sc.at[q, 0, 0], rc.at[q, k], {"dp": d}
                ).wait_recv()
        for i in range(few):
            for inside, away, local_copy in home_send(q, i):
                pl.when(jnp.logical_not(inside))(away.wait_send)
                pl.when(inside)(local_copy.wait)
        for j in order:
            for i in range(few):
                swap(q, j, i).wait_send()
            if j:
                ship_to(q, j).wait_send()

    lag = SPREAD_SKEW * (n - 2)
    later = [functools.partial(add_up, 0)]
    due = {
        ((r + 1) * per // 2 - 1) * blocks + (l + 1) * pairs - 1 + lag: (r, l)
        for r in (0, 1) for l in range(local)
    }
    for s in range(pieces + lag):
        for way in (0, 1):
            late = n - 2 - place[way]

            @pl.when((late >= 0) & (s == SPREAD_SKEW * late))
            def _():
                pass_on(shared, way, 0)

            i = s - SPREAD_SKEW * late

            @pl.when((late >= 0) & (i >= 0) & (i < pieces))
            def _():
                pass_on(routed, way, i)
        if s == lag:
            def _start():
                extra[2].wait()
                shared_gather()
            ready.append(_start)
            ready += [functools.partial(shared_down, c) for c in range(chunks)]
        if s in due:
            r, l = due[s]

            def _begin(r=r, l=l):
                if r == 0:
                    lowers[l].wait()
                gather(r, l)
            ready.append(_begin)
            for c in range(chunks):
                ready.append(functools.partial(routed_down, r, l, c))
                if l == local - 1 and r == 1 and spans[c][1] in (middle, width):
                    ready.append(functools.partial(swap_out, 1 if spans[c][1] == middle else 2))
            if l == local - 1 and r == 0:
                ready.append(functools.partial(swap_out, 0))
            if r == 1 and l == 0 and local > 2:
                ready.append(later.pop(0))
        quota = 3 if s < pieces + lag - 1 else len(ready)
        for task in ready[:quota]:
            task()
        ready = ready[quota:]

    for task in later:
        task()
    send_home(0)
    for stage_of in (add_up, send_home):
        for q in (1, 2):
            stage_of(q)
    for q in (0, 1, 2):
        arrive(q)

    def finish(group, way, i):
        @pl.when(place[way] < n - 1)
        def _():
            partial_send(group, way, i).wait_send()

        @pl.when(place[way] > 0)
        def _():
            hidden_send(group, way, i).wait_send()

    def drain(i, carry):
        for way in (0, 1):
            finish(routed, way, i)
        return carry

    lax.fori_loop(0, pieces, drain, 0)
    for way in (0, 1):
        finish(shared, way, 0)
    for copy in sends:
        copy.wait_send()


def layer(tokens, ids, weights, gate, up, down, sgate, sup, sdown, n, g):
    rows, model = tokens.shape
    width = model // n
    local, _, hidden = gate.shape
    experts = local * g
    thin = hidden // g
    wire = BF16 if n <= 4 else F32
    sliced = thin % 128 != 0
    if sliced:
        e = lax.axis_index("expert")
        sgate = lax.dynamic_slice_in_dim(sgate, e * thin, thin, 1)
        sup = lax.dynamic_slice_in_dim(sup, e * thin, thin, 1)
        sdown = lax.dynamic_slice_in_dim(sdown, e * thin, thin, 0)
    count = n * g * PITCH
    tiles = count // TILE
    slots = TILE // PITCH * CAP
    blocks = local * (hidden // COLS // 2)
    pieces = blocks * tiles * (slots // ROWS)
    half = n * g * rows // 2
    few = n // 4
    ring = min(AHEAD + 1, blocks)
    return pl.pallas_call(
        functools.partial(layer_kernel, n, g, sliced),
        out_shape=jax.ShapeDtypeStruct((rows, model), BF16),
        in_specs=[VMEM] * 3 + [HBM] * 6,
        out_specs=VMEM,
        scratch_shapes=[
            pltpu.VMEM((n, g, rows, width), BF16),
            pltpu.VMEM((n, g, rows, experts), F32),
            pltpu.VMEM((rows, experts), F32),
            pltpu.VMEM((count, width), BF16),
            pltpu.VMEM((count, experts), F32),
            pltpu.VMEM((ring, width, 2 * COLS), BF16),
            pltpu.VMEM((ring, width, 2 * COLS), BF16),
            pltpu.VMEM((local, hidden, width), BF16),
            pltpu.VMEM((width, thin), BF16),
            pltpu.VMEM((width, thin), BF16),
            pltpu.VMEM((thin, width), BF16),
            pltpu.VMEM((tiles, slots, width), BF16),
            pltpu.VMEM((TILE // PITCH * rows, width), BF16),
            pltpu.VMEM((count, hidden), BF16),
            pltpu.VMEM((count, thin), BF16),
            pltpu.VMEM((n * g, PITCH, width), F32),
            pltpu.VMEM((local, count, 1), F32),
            pltpu.VMEM((2, pieces, 2, ROWS, COLS), F32),
            pltpu.VMEM((2, pieces, 2, ROWS, COLS), wire),
            pltpu.VMEM((2, pieces, 2, ROWS, COLS) if wire == BF16 else (8, 128), wire),
            pltpu.VMEM((2, pieces, ROWS, COLS), BF16),
            pltpu.VMEM((2, 1, 2, half, thin), F32),
            pltpu.VMEM((2, 1, 2, half, thin), wire),
            pltpu.VMEM((2, 1, 2, half, thin), wire),
            pltpu.VMEM((2, 1, half, thin), BF16),
            pltpu.VMEM((tiles, local, slots, TILE), BF16),
            pltpu.VMEM((tiles * (slots // ROWS), local, 2 * ROWS, ROWS), BF16),
            pltpu.VMEM((2, g, few, PITCH, width), F32),
            pltpu.VMEM((2, few, rows, width), F32),
            pltpu.VMEM((2, g, few, rows, width), BF16),
            pltpu.VMEM((2, g, few, rows, width), BF16),
            pltpu.VMEM((2, few, rows, width), BF16),
            DMA((2, blocks)), DMA((local,)), DMA((3,)),
            DMA((2, pieces)), DMA((2, pieces)), DMA((2, pieces)), DMA((2, pieces)),
            DMA((2, 1)), DMA((2, 1)), DMA((2, 1)), DMA((2, 1)),
            DMA((2,)), DMA((2, n)), DMA((2, n)), DMA((2, n, g)), DMA((2, n, g)), DMA((n, g)), DMA((n, g)),
            DMA((3, g, few)), DMA((3, g, few)), DMA((3, g)), DMA((3, g)),
            DMA((3, few, 2)), DMA((3, n)), DMA((3,)),
        ],
        compiler_params=pltpu.CompilerParams(
            collective_id=0, has_side_effects=True, vmem_limit_bytes=67043328
        ),
    )(tokens, ids, weights, gate, up, down, sgate, sup, sdown)


def per_device(
    tokens, expert_ids, route_weights, gate_weights, up_weights, down_weights,
    shared_gate, shared_up, shared_down,
):
    g, n = lax.axis_size("expert"), lax.axis_size("dp")
    return layer(
        tokens, expert_ids.T, route_weights.T, gate_weights, up_weights, down_weights,
        shared_gate, shared_up, shared_down, n, g,
    )


def solution(mesh):
    placed = (
        P(("dp", "expert"), None),
        P(("dp", "expert"), None),
        P(("dp", "expert"), None),
        P("expert", "dp", "tensor"),
        P("expert", "dp", "tensor"),
        P("expert", "tensor", "dp"),
        P("dp", "tensor"),
        P("dp", "tensor"),
        P("tensor", "dp"),
    )
    return jax.shard_map(
        per_device, mesh=mesh, in_specs=placed, out_specs=P(("dp", "expert"), None), check_vma=False
    )
```
